128 devices in a mesh: ma: 16 (over x, y), row: 4 (over z_lo, core), col: 2 (over z_hi).
Axes of the slice: x: 4, y: 4, z: 4 (z_hi: 2, z_lo: 2; z = z_hi * 2 + z_lo), core: 2. Of those that a mesh axis runs over, the one named last changes fastest.
Arguments:
- foreground_cols: float32 [131072, 384], P('ma', ('row', 'col')), parts along dimension 0, as said below
- signal_rows: float32 [6144, 8192], P('ma', ('row', 'col')), parts along dimension 0, may hold values from -6 to 6
- visibilities: float32 [131072, 1024], P(('ma', 'row'), 'col'), parts along dimension 0, may hold values from -6 to 6
Outputs:
- factor_cols: float32 [131072, 384], P('ma', ('row', 'col')), parts along dimension 0
- whitened_rows: float32 [6144, 8192], P('ma', ('row', 'col')), parts along dimension 0
- projected: float32 [131072, 1024], P(('ma', 'row'), 'col'), parts along dimension 0
The draws below stay inside these ranges and needn't reach their ends.
There are 16 independent parts, one for each index of `ma`. The reference program is written for one: setup_inputs(seed, part) draws one part's arguments, and reference() takes and returns one part's arrays. A program takes and returns all parts, laid end to end along the dimension named above; each array names one. Nothing has to cross between parts.
Inputs may be any that keep to these rules, and one draw needn't show every extreme that they name: `foreground_cols`: the top 384 rows form a symmetric matrix whose eigenvalues are all 1 or more.
All inputs are finite; a program needn't handle non-finite values.
Results may differ from the reference program's by a relative error of at most 0.0001.
Values sent between devices are 32-bit elements; how exact they have to be, the bound alone decides.
A program may use at most 64 MiB of HBM per device.

```python
import jax
import jax.numpy as jnp
from jax import lax

N = 8192
CW = 48
W = 384
NVEC = 1024
N_ROW = 4
N_COL = 2


def draw_foreground_cols(key, part):
    key_g, key_d, key_r = jax.random.split(jax.random.fold_in(key, 7), 3)
    factors = jnp.clip(jax.random.normal(key_g, (W, W), jnp.float32), -4.0, 4.0)
    below = 0.25 * jnp.clip(jax.random.normal(key_r, (N - W, W), jnp.float32), -4.0, 4.0)
    diagonal = jnp.exp(jax.random.uniform(key_d, (W,), jnp.float32, 0.0, jnp.log(4.0)))
    top_block = jnp.dot(factors, factors.T, precision=lax.Precision.HIGHEST) / W + jnp.diag(diagonal)
    top_block = 0.5 * (top_block + top_block.T)
    return jnp.concatenate([top_block, below], axis=0)


def block_levels(stream_key, shape, cuts, smallest, largest):
    loudness = 1.0
    for position, blocks in cuts:
        heights = jax.random.uniform(jax.random.fold_in(jax.random.fold_in(stream_key, 6), position), (blocks,), jnp.float32, smallest / len(cuts), largest / len(cuts))
        loudness = loudness * jnp.repeat(jnp.exp(heights), shape[position] // blocks).reshape((-1,) + (1,) * (len(shape) - 1 - position))
    return loudness


def bell_draw(key, extent, deviation, most, cuts=(), dtype=jnp.bfloat16):
    array = jax.random.normal(key, extent, jnp.float32) * deviation
    if len(cuts) > 0:
        array = block_levels(key, extent, cuts, -0.22, 0.18) * array
    return jnp.clip(array, min=-most, max=most).astype(dtype)


def setup_inputs(seed: int = 0, part: int = 0) -> dict:
    arg_keys = jax.random.split(jax.random.key(seed), 4)
    own_keys = jax.random.split(jax.random.fold_in(arg_keys[3], part), 4)
    foreground_cols = draw_foreground_cols(jax.random.fold_in(jax.random.fold_in(arg_keys[3], part), 71), part)
    signal_rows = bell_draw(own_keys[1], (W, N), 1.0, 6.0, ((1, 8),), jnp.float32)
    visibilities = bell_draw(own_keys[2], (N, NVEC), 1.0, 6.0, ((0, 4), (1, 2)), jnp.float32)
    return dict(foreground_cols=foreground_cols, signal_rows=signal_rows, visibilities=visibilities)


def panel_of(column_block, first_row, panel_width):
    diag_part = lax.dynamic_slice_in_dim(column_block, first_row, panel_width, 0)
    diag_factor = jnp.linalg.cholesky(diag_part)
    solved = lax.linalg.triangular_solve(diag_factor, column_block, left_side=False, lower=True, transpose_a=True)
    row_ids = lax.broadcasted_iota(jnp.int32, column_block.shape, 0)
    solved = jnp.where(row_ids < first_row, jnp.zeros_like(solved), solved)
    return lax.dynamic_update_slice_in_dim(solved, diag_factor, first_row, 0)

def whiten_step(right_side, panel_cols, first_row, panel_width):
    diag_factor = lax.dynamic_slice_in_dim(panel_cols, first_row, panel_width, 0)
    head_rows = lax.dynamic_slice_in_dim(right_side, first_row, panel_width, 0)
    solved = lax.linalg.triangular_solve(diag_factor, head_rows, left_side=True, lower=True)
    remainder = right_side - jnp.dot(panel_cols[:right_side.shape[0]], solved, precision=lax.Precision.HIGHEST)
    return lax.dynamic_update_slice_in_dim(remainder, solved, first_row, 0)

def reference(foreground_cols, signal_rows, visibilities):
    panel_width = CW
    factor = foreground_cols
    whitened = signal_rows
    projected = visibilities
    for sweep_step in range(N_ROW * N_COL):
        first_row = sweep_step * panel_width
        next_row = first_row + panel_width
        panel_cols = panel_of(factor[:, first_row:next_row], first_row, panel_width)
        trailing = factor[:, next_row:] - jnp.dot(panel_cols, panel_cols[next_row:W].T, precision=lax.Precision.HIGHEST)
        factor = jnp.concatenate([factor[:, :first_row], panel_cols, trailing], axis=1)
        whitened = whiten_step(whitened, panel_cols, first_row, panel_width)
        projected = whiten_step(projected, panel_cols, first_row, panel_width)
    return (factor, whitened, projected)
```

```python
import jax
import jax.numpy as jnp
from jax import lax
from jax.experimental import pallas as pl
from jax.experimental.pallas import tpu as pltpu
from jax.sharding import PartitionSpec as P

MESH = pl.DeviceIdType.MESH
F32 = jnp.float32
B = 128
HI = lax.Precision.HIGHEST

def dot(a, b, dims=((1,), (0,))):
    return lax.dot_general(a, b, (dims, ((), ())), precision=HI, preferred_element_type=jnp.float32)

def diag_block(d_ref, e_ref):
    for p in range(B // 8):
        c0 = 8 * p
        rows = pl.ds(c0, 8)
        panel = d_ref[rows, :]
        cols = [jnp.broadcast_to(panel[:, c0 + j:c0 + j + 1], (8, B)) for j in range(8)]
        s = {(i, j): jnp.broadcast_to(cols[j][i:i + 1, :], (8, B)) for j in range(8) for i in range(j, 8)}
        w = [jnp.broadcast_to(panel[i:i + 1, :], (8, B)) for i in range(8)]
        ep = e_ref[rows, :]
        v = [jnp.broadcast_to(ep[i:i + 1, :], (8, B)) for i in range(8)]
        r = []
        for j in range(8):
            r.append(lax.rsqrt(s[j, j]))
            for i in range(j + 1, 8):
                s[i, j] = s[i, j] * r[j]
            for k in range(j + 1, 8):
                for i in range(k, 8):
                    s[i, k] = s[i, k] - s[i, j] * s[k, j]
            w[j] = w[j] * r[j]
            v[j] = v[j] * r[j]
            for i in range(j + 1, 8):
                w[i] = w[i] - s[i, j] * w[j]
                v[i] = v[i] - s[i, j] * v[j]
        for j in range(8):
            d_ref[pl.ds(c0 + j, 1), :] = w[j][:1]
            e_ref[pl.ds(c0 + j, 1), :] = v[j][:1]
        for q in range(p + 1, B // 8):
            rq = pl.ds(8 * q, 8)
            dq = d_ref[rq, :]
            eq = e_ref[rq, :]
            g = [jnp.broadcast_to(dq[:, c0 + j:c0 + j + 1], (8, B)) for j in range(8)]
            for j in range(8):
                g[j] = g[j] * r[j]
                for k in range(j + 1, 8):
                    g[k] = g[k] - g[j] * s[k, j]
                dq = dq - g[j] * w[j]
                eq = eq - g[j] * v[j]
            d_ref[rq, :] = dq
            e_ref[rq, :] = eq

def factor(a_ref, e_ref, d_ref, f_ref):
    n = a_ref.shape[0]
    eye = (lax.broadcasted_iota(jnp.int32, (n, n), 0) == lax.broadcasted_iota(jnp.int32, (n, n), 1))
    e_ref[...] = eye.astype(jnp.float32)
    def step(b, _):
        blk = pl.ds(pl.multiple_of(b * B, B), B)
        d_ref[...] = a_ref[blk, blk]
        f_ref[...] = eye[:B, :B].astype(jnp.float32)
        diag_block(d_ref, f_ref)
        inv = f_ref[...]
        below = lax.broadcasted_iota(jnp.int32, (n, B), 0) >= (b + 1) * B
        left = jnp.where(below, dot(a_ref[:, blk], inv, ((1,), (1,))), 0.0)
        top = dot(inv, a_ref[blk, :])
        etop = dot(inv, e_ref[blk, :])
        a_ref[...] = a_ref[...] - dot(left, top)
        e_ref[...] = e_ref[...] - dot(left, etop)
        a_ref[blk, :] = top
        e_ref[blk, :] = etop
        a_ref[blk, blk] = d_ref[...]
        return 0
    lax.fori_loop(0, n // B, step, 0)
    upper = lax.broadcasted_iota(jnp.int32, (n, n), 0) <= lax.broadcasted_iota(jnp.int32, (n, n), 1)
    a_ref[...] = jnp.where(upper, a_ref[...], 0.0)


PEERS = ((1, 0), (3, 0), (2, 0), (1, 1), (3, 1), (2, 1), (0, 1))
NEAR = ((1, 0), (3, 0), (1, 1), (3, 1))


def rows_of(start, size, unit):
    return pl.ds(pl.multiple_of(start, unit), size)


def kernel(ct_hbm, s_hbm, v_hbm, ft, wh, pr,
           ct, cr, s, v, vt, square, a, e, d, f, y, zv, own, other,
           load_sem, top_s, top_r, col_s, col_r, vec_s, vec_r, back_s, back_r):
    width, length = ct.shape
    n = square.shape[0]
    span = v.shape[0]
    half = span // 2
    nh = n // 2
    row, col = lax.axis_index("row"), lax.axis_index("col")
    lo, core = row // 2, row % 2
    z = col * 2 + lo
    member = row * 2 + col

    def place(dz, dc):
        zz, cc = (z + dz) % 4, (core + dc) % 2
        return (zz % 2) * 2 + cc, zz // 2

    def peer(dz, dc):
        r, c = place(dz, dc)
        return {"row": r, "col": c}

    def remote(src, dst, send, recv, to):
        return pltpu.make_async_remote_copy(
            src_ref=src, dst_ref=dst, send_sem=send, recv_sem=recv, device_id=to, device_id_type=MESH
        )

    mine = rows_of(member * width, width, 8)
    top_load = pltpu.make_async_copy(ct_hbm.at[:, pl.ds(0, n)], square.at[mine, :], load_sem.at[0])
    ct_load = pltpu.make_async_copy(ct_hbm, ct, load_sem.at[1])
    cr_load = pltpu.make_async_copy(
        ct_hbm.at[:, rows_of(row * span, span, 128)], cr.at[mine, :], load_sem.at[2]
    )
    s_load = pltpu.make_async_copy(s_hbm, s, load_sem.at[3])
    v_load = pltpu.make_async_copy(v_hbm, v, load_sem.at[4])
    for load in (top_load, ct_load, cr_load, v_load, s_load):
        load.start()

    barrier = pltpu.get_barrier_semaphore()
    for dz, dc in PEERS:
        pl.semaphore_signal(barrier, inc=1, device_id=peer(dz, dc), device_id_type=MESH)
    pl.semaphore_wait(barrier, len(PEERS))

    top_load.wait()
    tops = []
    for i, (dz, dc) in enumerate(PEERS):
        copy = remote(square.at[mine, :], square.at[mine, :], top_s.at[i], top_r.at[i], peer(dz, dc))
        copy.start()
        tops.append(copy)
    ct_load.wait()
    cols = []
    for i, (dz, dc) in enumerate(PEERS):
        r, _ = place(dz, dc)
        copy = remote(
            ct.at[:, rows_of(r * span, span, 128)], cr.at[mine, :], col_s.at[i], col_r.at[i], peer(dz, dc)
        )
        copy.start()
        cols.append(copy)

    v_load.wait()
    first, second = pl.ds(0, nh), pl.ds(nh, nh)
    to_core = remote(v.at[pl.ds(0, n), :], vt, vec_s.at[0], vec_r.at[0], {"row": 1, "col": col})
    to_first = remote(v.at[first, :], vt.at[first, :], vec_s.at[1], vec_r.at[1], {"row": 2, "col": col})
    to_second = remote(v.at[second, :], vt.at[second, :], vec_s.at[2], vec_r.at[1], {"row": 3, "col": col})
    pass_first = remote(vt.at[first, :], vt.at[first, :], vec_s.at[0], vec_r.at[0], {"row": 3, "col": col})
    pass_second = remote(vt.at[second, :], vt.at[second, :], vec_s.at[0], vec_r.at[0], {"row": 2, "col": col})

    @pl.when(row == 0)
    def _():
        to_core.start()
        to_first.start()
        to_second.start()
        vt[...] = v[pl.ds(0, n), :]

    for copy in tops:
        copy.wait()
    a[...] = square[...]
    factor(a, e, d, f)
    inverse = e[...]

    s_load.wait()
    wh[...] = dot(inverse, s[...])

    @pl.when(row == 2)
    def _():
        to_first.wait_recv()
        pass_first.start()
        pass_second.wait_recv()

    @pl.when(row == 3)
    def _():
        to_second.wait_recv()
        pass_second.start()
        pass_first.wait_recv()

    @pl.when(row == 1)
    def _():
        to_core.wait_recv()

    y[...] = dot(inverse, vt[...])
    zv[...] = dot(inverse.T, y[...])

    cr_load.wait()
    for copy in cols:
        copy.wait_recv()
    block = rows_of(row * span + col * half, half, 128)
    other[...] = dot(e[rows_of((1 - lo) * nh, nh, 8), :], cr[:, rows_of(col * half, half, 128)])
    backs = []
    for i, (dz, dc) in enumerate(NEAR):
        r, c = place(dz, dc)
        copy = remote(
            other.at[rows_of((r % 2) * 2 * width + c * width, width, 8), :],
            ft.at[:, block], back_s.at[i], back_r.at[i], peer(dz, dc),
        )
        copy.start()
        backs.append(copy)
    for j in range(2):
        rows = rows_of(((lo * 2 + (core + j) % 2) * 2 + col) * width, width, 8)
        own[pl.ds(j * width, width), :] = e[rows, :]
    kept = dot(own[...], cr[...])
    ft[:, rows_of(row * span, span, 128)] = kept[:width]
    give_ref = ct
    for copy in cols:
        copy.wait_send()
    give_ref[:, pl.ds(0, span)] = kept[width:]
    copy = remote(
        give_ref.at[:, pl.ds(0, span)], ft.at[:, rows_of(row * span, span, 128)],
        back_s.at[4], back_r.at[4], peer(0, 1),
    )
    copy.start()
    backs.append(copy)

    step = 256

    def project(i, _):
        part = rows_of(i * step, step, 128)
        pr[part, :] = v[part, :] - dot(cr[:, part].T, zv[...])
        return 0

    lax.fori_loop(0, span // step, project, 0)

    @pl.when(row == 0)
    def _():
        to_core.wait_send()
        to_first.wait_send()
        to_second.wait_send()
        pr[pl.ds(0, n), :] = y[...]

    @pl.when(row == 2)
    def _():
        pass_first.wait_send()

    @pl.when(row == 3)
    def _():
        pass_second.wait_send()

    for copy in backs:
        copy.wait()
    ft[:, pl.ds(0, n)] = a[mine, :]


def shards(foreground_cols, signal_rows, visibilities):
    length, width = foreground_cols.shape
    n = signal_rows.shape[0]
    span, vecs = visibilities.shape
    vmem = pl.BlockSpec(memory_space=pltpu.VMEM)
    hbm = pl.BlockSpec(memory_space=pl.ANY)
    dma = pltpu.SemaphoreType.DMA
    buffers = (
        (width, length), (n, span), signal_rows.shape, visibilities.shape, (n, vecs), (n, n), (n, n), (n, n),
        (B, B), (B, B), (n, vecs), (n, vecs), (2 * width, n), (n // 2, span // 2),
    )
    ft, whitened, projected = pl.pallas_call(
        kernel,
        name="whiten",
        out_shape=[
            jax.ShapeDtypeStruct((width, length), F32),
            jax.ShapeDtypeStruct(signal_rows.shape, F32),
            jax.ShapeDtypeStruct(visibilities.shape, F32),
        ],
        in_specs=[hbm] * 3,
        out_specs=[vmem] * 3,
        scratch_shapes=[pltpu.VMEM(shape, F32) for shape in buffers]
        + [dma((k,)) for k in (5, 7, 7, 7, 7, 3, 2, 5, 5)],
        compiler_params=pltpu.CompilerParams(
            collective_id=0, has_side_effects=True, vmem_limit_bytes=60 * 1024 * 1024
        ),
    )(foreground_cols.T, signal_rows, visibilities)
    return ft.T, whitened, projected


def solution(mesh):
    return jax.shard_map(
        shards,
        mesh=mesh,
        in_specs=(P("ma", ("row", "col")), P("ma", ("row", "col")), P(("ma", "row"), "col")),
        out_specs=(P("ma", ("row", "col")), P("ma", ("row", "col")), P(("ma", "row"), "col")),
        check_vma=False,
    )
```

```python
import jax
import jax.numpy as jnp
from jax import lax
from jax.experimental import pallas as pl
from jax.experimental.pallas import tpu as pltpu
from jax.sharding import PartitionSpec as P

MESH = pl.DeviceIdType.MESH
F32 = jnp.float32
B = 128
HI = lax.Precision.HIGHEST

def dot(a, b, dims=((1,), (0,))):
    return lax.dot_general(a, b, (dims, ((), ())), precision=HI, preferred_element_type=jnp.float32)

def diag_block(d_ref, e_ref):
    for p in range(B // 8):
        c0 = 8 * p
        rows = pl.ds(c0, 8)
        panel = d_ref[rows, :]
        cols = [jnp.broadcast_to(panel[:, c0 + j:c0 + j + 1], (8, B)) for j in range(8)]
        s = {(i, j): jnp.broadcast_to(cols[j][i:i + 1, :], (8, B)) for j in range(8) for i in range(j, 8)}
        w = [jnp.broadcast_to(panel[i:i + 1, :], (8, B)) for i in range(8)]
        ep = e_ref[rows, :]
        v = [jnp.broadcast_to(ep[i:i + 1, :], (8, B)) for i in range(8)]
        r = []
        for j in range(8):
            r.append(lax.rsqrt(s[j, j]))
            for i in range(j + 1, 8):
                s[i, j] = s[i, j] * r[j]
            for k in range(j + 1, 8):
                for i in range(k, 8):
                    s[i, k] = s[i, k] - s[i, j] * s[k, j]
            w[j] = w[j] * r[j]
            v[j] = v[j] * r[j]
            for i in range(j + 1, 8):
                w[i] = w[i] - s[i, j] * w[j]
                v[i] = v[i] - s[i, j] * v[j]
        for j in range(8):
            d_ref[pl.ds(c0 + j, 1), :] = w[j][:1]
            e_ref[pl.ds(c0 + j, 1), :] = v[j][:1]
        for q in range(p + 1, B // 8):
            rq = pl.ds(8 * q, 8)
            dq = d_ref[rq, :]
            eq = e_ref[rq, :]
            g = [jnp.broadcast_to(dq[:, c0 + j:c0 + j + 1], (8, B)) for j in range(8)]
            for j in range(8):
                g[j] = g[j] * r[j]
                for k in range(j + 1, 8):
                    g[k] = g[k] - g[j] * s[k, j]
                dq = dq - g[j] * w[j]
                eq = eq - g[j] * v[j]
            d_ref[rq, :] = dq
            e_ref[rq, :] = eq

def factor(a_ref, e_ref, d_ref, f_ref):
    n = a_ref.shape[0]
    eye = (lax.broadcasted_iota(jnp.int32, (n, n), 0) == lax.broadcasted_iota(jnp.int32, (n, n), 1))
    e_ref[...] = eye.astype(jnp.float32)
    def step(b, _):
        blk = pl.ds(pl.multiple_of(b * B, B), B)
        d_ref[...] = a_ref[blk, blk]
        f_ref[...] = eye[:B, :B].astype(jnp.float32)
        diag_block(d_ref, f_ref)
        inv = f_ref[...]
        below = lax.broadcasted_iota(jnp.int32, (n, B), 0) >= (b + 1) * B
        left = jnp.where(below, dot(a_ref[:, blk], inv, ((1,), (1,))), 0.0)
        top = dot(inv, a_ref[blk, :])
        etop = dot(inv, e_ref[blk, :])
        a_ref[...] = a_ref[...] - dot(left, top)
        e_ref[...] = e_ref[...] - dot(left, etop)
        a_ref[blk, :] = top
        e_ref[blk, :] = etop
        a_ref[blk, blk] = d_ref[...]
        return 0
    lax.fori_loop(0, n // B, step, 0)
    upper = lax.broadcasted_iota(jnp.int32, (n, n), 0) <= lax.broadcasted_iota(jnp.int32, (n, n), 1)
    a_ref[...] = jnp.where(upper, a_ref[...], 0.0)


PEERS = ((1, 0), (3, 0), (2, 0), (1, 1), (3, 1), (2, 1), (0, 1))
FAR = ((1, 0), (3, 0), (2, 0))
NEAR = ((1, 0), (3, 0), (1, 1), (3, 1))


def rows_of(start, size, unit):
    return pl.ds(pl.multiple_of(start, unit), size)


def kernel(ct_hbm, s_hbm, v_hbm, ft, wh, pr,
           ct, cr, s, v, vt, square, a, e, d, f, y, zv, left, near, own,
           load_sem, top_s, top_r, pass_s, pass_r, col_s, col_r, vec_s, vec_r, back_s, back_r):
    width, length = ct.shape
    n = square.shape[0]
    span = v.shape[0]
    half = span // 2
    nh = n // 2
    row, col = lax.axis_index("row"), lax.axis_index("col")
    lo, core = row // 2, row % 2
    z = col * 2 + lo

    def place(dz, dc):
        zz, cc = (z + dz) % 4, (core + dc) % 2
        return (zz % 2) * 2 + cc, zz // 2

    def peer(dz, dc):
        r, c = place(dz, dc)
        return {"row": r, "col": c}

    def band(dz, dc):
        r, c = place(dz, dc)
        return rows_of((r * 2 + c) * width, width, 8)

    def remote(src, dst, send, recv, to):
        return pltpu.make_async_remote_copy(
            src_ref=src, dst_ref=dst, send_sem=send, recv_sem=recv, device_id=to, device_id_type=MESH
        )

    mine = band(0, 0)
    top_load = pltpu.make_async_copy(ct_hbm.at[:, pl.ds(0, n)], square.at[mine, :], load_sem.at[0])
    ct_load = pltpu.make_async_copy(ct_hbm, ct, load_sem.at[1])
    cr_load = pltpu.make_async_copy(
        ct_hbm.at[:, rows_of(row * span, span, 128)], cr.at[mine, :], load_sem.at[2]
    )
    v_load = pltpu.make_async_copy(v_hbm, v, load_sem.at[3])
    s_load = pltpu.make_async_copy(s_hbm, s, load_sem.at[4])
    for load in (top_load, ct_load, cr_load, v_load, s_load):
        load.start()

    barrier = pltpu.get_barrier_semaphore()
    for dz, dc in PEERS:
        pl.semaphore_signal(barrier, inc=1, device_id=peer(dz, dc), device_id_type=MESH)
    pl.semaphore_wait(barrier, len(PEERS))

    top_load.wait()
    tops, passes = [], []
    for i, (dz, dc) in enumerate(FAR):
        tops.append(remote(square.at[mine, :], square.at[mine, :], top_s.at[i], top_r.at[i], peer(dz, dc)))
    for i, (dz, dc) in enumerate(FAR + ((0, 0),)):
        block = square.at[band(-dz, dc), :]
        passes.append(remote(block, block, pass_s.at[i], pass_r.at[i], peer(0, 1)))
    for copy in tops:
        copy.start()
    passes[3].start()

    ct_load.wait()
    cols = [[], []]
    for turn in range(2):
        for i, (dz, dc) in enumerate(PEERS):
            r, c = place(dz, dc)
            which = c if turn == 0 else 1 - c
            copy = remote(
                ct.at[:, rows_of(r * span + which * half, half, 128)],
                cr.at[mine, rows_of(which * half, half, 128)],
                col_s.at[turn, i], col_r.at[turn, i], peer(dz, dc),
            )
            cols[turn].append(copy)
    for copy in cols[0]:
        copy.start()

    v_load.wait()
    first, second = pl.ds(0, nh), pl.ds(nh, nh)
    to_core = remote(v.at[pl.ds(0, n), :], vt, vec_s.at[0], vec_r.at[0], {"row": 1, "col": col})
    to_first = remote(v.at[first, :], vt.at[first, :], vec_s.at[1], vec_r.at[1], {"row": 2, "col": col})
    to_second = remote(v.at[second, :], vt.at[second, :], vec_s.at[2], vec_r.at[1], {"row": 3, "col": col})
    pass_first = remote(vt.at[first, :], vt.at[first, :], vec_s.at[0], vec_r.at[0], {"row": 3, "col": col})
    pass_second = remote(vt.at[second, :], vt.at[second, :], vec_s.at[0], vec_r.at[0], {"row": 2, "col": col})

    @pl.when(row == 0)
    def _():
        to_core.start()
        to_first.start()
        to_second.start()
        vt[...] = v[pl.ds(0, n), :]

    for copy in cols[1]:
        copy.start()

    for i in range(3):
        tops[i].wait_recv()
        passes[i].start()
    for copy in passes:
        copy.wait()
    for copy in tops:
        copy.wait_send()
    a[...] = square[...]
    factor(a, e, d, f)
    inverse = e[...]

    s_load.wait()
    wh[...] = dot(inverse, s[...])

    @pl.when(row == 2)
    def _():
        to_first.wait_recv()
        pass_first.start()
        pass_second.wait_recv()

    @pl.when(row == 3)
    def _():
        to_second.wait_recv()
        pass_second.start()
        pass_first.wait_recv()

    @pl.when(row == 1)
    def _():
        to_core.wait_recv()

    left[pl.ds(0, nh), :] = e[rows_of((1 - lo) * nh, nh, 8), :]
    for j in range(2):
        left[pl.ds(nh + j * width, width), :] = e[band(0, j), :]

    cr_load.wait()
    for copy in cols[0]:
        copy.wait_recv()
    here, there = rows_of(col * half, half, 128), rows_of((1 - col) * half, half, 128)
    here_out = rows_of(row * span + col * half, half, 128)
    there_out = rows_of(row * span + (1 - col) * half, half, 128)
    near[...] = dot(left[pl.ds(0, nh), :], cr[:, here])
    backs = []
    for i, (dz, dc) in enumerate(NEAR):
        r, c = place(dz, dc)
        copy = remote(
            near.at[rows_of((r % 2) * 2 * width + c * width, width, 8), :],
            ft.at[:, here_out], back_s.at[i], back_r.at[i], peer(dz, dc),
        )
        copy.start()
        backs.append(copy)
    kept = dot(left[pl.ds(nh, 2 * width), :], cr[:, here])
    ft[:, here_out] = kept[:width]
    own[0, :, :] = kept[width:]
    copy = remote(own.at[0], ft.at[:, here_out], back_s.at[4], back_r.at[4], peer(0, 1))
    copy.start()
    backs.append(copy)

    y[...] = dot(inverse, vt[...])
    zv[...] = dot(inverse.T, y[...])

    step = 256

    def project(start):
        def body(i, _):
            part = rows_of(start + i * step, step, 128)
            pr[part, :] = v[part, :] - dot(cr[:, part].T, zv[...])
            return 0

        lax.fori_loop(0, half // step, body, 0)

    project(col * half)

    for copy in cols[1]:
        copy.wait_recv()
    kept = dot(left[pl.ds(nh, 2 * width), :], cr[:, there])
    ft[:, there_out] = kept[:width]
    own[1, :, :] = kept[width:]
    copy = remote(own.at[1], ft.at[:, there_out], back_s.at[5], back_r.at[5], peer(0, 1))
    copy.start()
    backs.append(copy)

    project((1 - col) * half)

    @pl.when(row == 0)
    def _():
        to_core.wait_send()
        to_first.wait_send()
        to_second.wait_send()
        pr[pl.ds(0, n), :] = y[...]

    @pl.when(row == 2)
    def _():
        pass_first.wait_send()

    @pl.when(row == 3)
    def _():
        pass_second.wait_send()

    for copy in cols[0] + cols[1]:
        copy.wait_send()
    for copy in backs:
        copy.wait()
    ft[:, pl.ds(0, n)] = a[mine, :]


def shards(foreground_cols, signal_rows, visibilities):
    length, width = foreground_cols.shape
    n = signal_rows.shape[0]
    span, vecs = visibilities.shape
    vmem = pl.BlockSpec(memory_space=pltpu.VMEM)
    hbm = pl.BlockSpec(memory_space=pl.ANY)
    dma = pltpu.SemaphoreType.DMA
    buffers = (
        (width, length), (n, span), signal_rows.shape, visibilities.shape, (n, vecs), (n, n), (n, n), (n, n),
        (B, B), (B, B), (n, vecs), (n, vecs), (n // 2 + 2 * width, n), (n // 2, span // 2), (2, width, span // 2),
    )
    ft, whitened, projected = pl.pallas_call(
        kernel,
        name="whiten",
        out_shape=[
            pltpu.VMEM((width, length), F32),
            pltpu.VMEM(signal_rows.shape, F32),
            pltpu.VMEM(visibilities.shape, F32),
        ],
        in_specs=[hbm] * 3,
        out_specs=[vmem] * 3,
        scratch_shapes=[pltpu.VMEM(shape, F32) for shape in buffers]
        + [dma(k) for k in ((5,), (3,), (3,), (4,), (4,), (2, 7), (2, 7), (3,), (2,), (6,), (6,))],
        compiler_params=pltpu.CompilerParams(
            collective_id=0, has_side_effects=True, vmem_limit_bytes=56 * 1024 * 1024
        ),
    )(foreground_cols.T, signal_rows, visibilities)
    return ft.T, whitened, projected


def solution(mesh):
    return jax.shard_map(
        shards,
        mesh=mesh,
        in_specs=(P("ma", ("row", "col")), P("ma", ("row", "col")), P(("ma", "row"), "col")),
        out_specs=(P("ma", ("row", "col")), P("ma", ("row", "col")), P(("ma", "row"), "col")),
        check_vma=False,
    )
```

```python
import jax
import jax.numpy as jnp
from jax import lax
from jax.experimental import pallas as pl
from jax.experimental.pallas import tpu as pltpu
from jax.sharding import PartitionSpec as P

MESH = pl.DeviceIdType.MESH
F32 = jnp.float32
B = 128
HI = lax.Precision.HIGHEST

def dot(a, b, dims=((1,), (0,))):
    return lax.dot_general(a, b, (dims, ((), ())), precision=HI, preferred_element_type=jnp.float32)

def diag_block(d_ref, e_ref):
    for p in range(B // 8):
        c0 = 8 * p
        rows = pl.ds(c0, 8)
        panel = d_ref[rows, :]
        cols = [jnp.broadcast_to(panel[:, c0 + j:c0 + j + 1], (8, B)) for j in range(8)]
        s = {(i, j): jnp.broadcast_to(cols[j][i:i + 1, :], (8, B)) for j in range(8) for i in range(j, 8)}
        w = [jnp.broadcast_to(panel[i:i + 1, :], (8, B)) for i in range(8)]
        ep = e_ref[rows, :]
        v = [jnp.broadcast_to(ep[i:i + 1, :], (8, B)) for i in range(8)]
        r = []
        for j in range(8):
            r.append(lax.rsqrt(s[j, j]))
            for i in range(j + 1, 8):
                s[i, j] = s[i, j] * r[j]
            for k in range(j + 1, 8):
                for i in range(k, 8):
                    s[i, k] = s[i, k] - s[i, j] * s[k, j]
            w[j] = w[j] * r[j]
            v[j] = v[j] * r[j]
            for i in range(j + 1, 8):
                w[i] = w[i] - s[i, j] * w[j]
                v[i] = v[i] - s[i, j] * v[j]
        for j in range(8):
            d_ref[pl.ds(c0 + j, 1), :] = w[j][:1]
            e_ref[pl.ds(c0 + j, 1), :] = v[j][:1]
        for q in range(p + 1, B // 8):
            rq = pl.ds(8 * q, 8)
            dq = d_ref[rq, :]
            eq = e_ref[rq, :]
            g = [jnp.broadcast_to(dq[:, c0 + j:c0 + j + 1], (8, B)) for j in range(8)]
            for j in range(8):
                g[j] = g[j] * r[j]
                for k in range(j + 1, 8):
                    g[k] = g[k] - g[j] * s[k, j]
                dq = dq - g[j] * w[j]
                eq = eq - g[j] * v[j]
            d_ref[rq, :] = dq
            e_ref[rq, :] = eq

def factor(a_ref, e_ref, d_ref, f_ref):
    n = a_ref.shape[0]
    eye = (lax.broadcasted_iota(jnp.int32, (n, n), 0) == lax.broadcasted_iota(jnp.int32, (n, n), 1))
    e_ref[...] = eye.astype(jnp.float32)
    def step(b, _):
        blk = pl.ds(pl.multiple_of(b * B, B), B)
        d_ref[...] = a_ref[blk, blk]
        f_ref[...] = eye[:B, :B].astype(jnp.float32)
        diag_block(d_ref, f_ref)
        inv = f_ref[...]
        below = lax.broadcasted_iota(jnp.int32, (n, B), 0) >= (b + 1) * B
        left = jnp.where(below, dot(a_ref[:, blk], inv, ((1,), (1,))), 0.0)
        top = dot(inv, a_ref[blk, :])
        etop = dot(inv, e_ref[blk, :])
        a_ref[...] = a_ref[...] - dot(left, top)
        e_ref[...] = e_ref[...] - dot(left, etop)
        a_ref[blk, :] = top
        e_ref[blk, :] = etop
        a_ref[blk, blk] = d_ref[...]
        return 0
    lax.fori_loop(0, n // B, step, 0)
    upper = lax.broadcasted_iota(jnp.int32, (n, n), 0) <= lax.broadcasted_iota(jnp.int32, (n, n), 1)
    a_ref[...] = jnp.where(upper, a_ref[...], 0.0)


PEERS = ((1, 0), (3, 0), (2, 0), (1, 1), (3, 1), (2, 1), (0, 1))
FAR = ((1, 0), (3, 0), (2, 0))


def rows_of(start, size, unit):
    return pl.ds(pl.multiple_of(start, unit), size)


def split(x):
    high = x.astype(jnp.bfloat16)
    return high, (x - high.astype(F32)).astype(jnp.bfloat16)


def dot3(a, b):
    def one(x, y):
        return lax.dot_general(x, y, (((1,), (0,)), ((), ())), preferred_element_type=F32)

    return one(a[0], b[0]) + (one(a[0], b[1]) + one(a[1], b[0]))


def kernel(ct_hbm, s_hbm, v_hbm, ft, wh, pr,
           ct, cr, s, v, vt, square, a, e, d, f, y, zv, left, near, own,
           load_sem, top_s, top_r, pass_s, pass_r, col_s, col_r, vec_s, vec_r, back_s, back_r, give_s, give_r):
    width, length = ct.shape
    n = square.shape[0]
    span = v.shape[0]
    half = span // 2
    nh = n // 2
    row, col = lax.axis_index("row"), lax.axis_index("col")
    lo, core = row // 2, row % 2
    z = col * 2 + lo

    def place(dz, dc):
        zz, cc = (z + dz) % 4, (core + dc) % 2
        return (zz % 2) * 2 + cc, zz // 2

    def peer(dz, dc):
        r, c = place(dz, dc)
        return {"row": r, "col": c}

    def band(dz, dc):
        r, c = place(dz, dc)
        return rows_of((r * 2 + c) * width, width, 8)

    def remote(src, dst, send, recv, to):
        return pltpu.make_async_remote_copy(
            src_ref=src, dst_ref=dst, send_sem=send, recv_sem=recv, device_id=to, device_id_type=MESH
        )

    mine = band(0, 0)
    top_load = pltpu.make_async_copy(ct_hbm.at[:, pl.ds(0, n)], square.at[mine, :], load_sem.at[0])
    ct_load = pltpu.make_async_copy(ct_hbm, ct, load_sem.at[1])
    cr_load = pltpu.make_async_copy(
        ct_hbm.at[:, rows_of(row * span, span, 128)], cr.at[mine, :], load_sem.at[2]
    )
    v_load = pltpu.make_async_copy(v_hbm, v, load_sem.at[3])
    s_load = pltpu.make_async_copy(s_hbm, s, load_sem.at[4])
    for load in (top_load, ct_load, cr_load, v_load, s_load):
        load.start()

    barrier = pltpu.get_barrier_semaphore()
    for dz, dc in PEERS:
        pl.semaphore_signal(barrier, inc=1, device_id=peer(dz, dc), device_id_type=MESH)
    pl.semaphore_wait(barrier, len(PEERS))

    top_load.wait()
    tops, passes = [], []
    for i, (dz, dc) in enumerate(FAR):
        tops.append(remote(square.at[mine, :], square.at[mine, :], top_s.at[i], top_r.at[i], peer(dz, dc)))
    for i, (dz, dc) in enumerate(FAR + ((0, 0),)):
        block = square.at[band(-dz, dc), :]
        passes.append(remote(block, block, pass_s.at[i], pass_r.at[i], peer(0, 1)))
    for copy in tops:
        copy.start()
    passes[3].start()

    ct_load.wait()
    quarter = half // 2
    cols = [[], [], []]
    for turn, size in enumerate((half, quarter, quarter)):
        for i, (dz, dc) in enumerate(PEERS):
            r, c = place(dz, dc)
            early = (r // 2) * c
            start = early * half if turn == 0 else (1 - early) * half + (turn - 1) * quarter
            cols[turn].append(remote(
                ct.at[:, rows_of(r * span + start, size, 128)], cr.at[mine, rows_of(start, size, 128)],
                col_s.at[turn, i], col_r.at[turn, i], peer(dz, dc),
            ))
    for copy in cols[0]:
        copy.start()

    v_load.wait()
    first, second = pl.ds(0, nh), pl.ds(nh, nh)
    to_core = remote(v.at[pl.ds(0, n), :], vt, vec_s.at[0], vec_r.at[0], {"row": 1, "col": col})
    to_first = remote(v.at[first, :], vt.at[first, :], vec_s.at[1], vec_r.at[1], {"row": 2, "col": col})
    to_second = remote(v.at[second, :], vt.at[second, :], vec_s.at[2], vec_r.at[1], {"row": 3, "col": col})
    pass_first = remote(vt.at[first, :], vt.at[first, :], vec_s.at[0], vec_r.at[0], {"row": 3, "col": col})
    pass_second = remote(vt.at[second, :], vt.at[second, :], vec_s.at[0], vec_r.at[0], {"row": 2, "col": col})

    @pl.when(row == 0)
    def _():
        to_core.start()
        to_first.start()
        to_second.start()
        vt[...] = v[pl.ds(0, n), :]

    for copy in cols[1] + cols[2]:
        copy.start()

    for i in range(3):
        tops[i].wait_recv()
        passes[i].start()
    for copy in passes:
        copy.wait()
    for copy in tops:
        copy.wait_send()
    a[...] = square[...]
    factor(a, e, d, f)
    left[pl.ds(0, nh), :] = e[rows_of((1 - lo) * nh, nh, 8), :]
    for j in range(2):
        left[pl.ds(nh + j * width, width), :] = e[band(0, j), :]

    cr_load.wait()
    for copy in cols[0]:
        copy.wait_recv()
    early = lo * col
    base = row * span
    lefts = split(left[...])
    def back(dz, dc, kind, start, size):
        r, c = place(dz, dc)
        return remote(
            near.at[rows_of((r % 2) * 2 * width + c * width, width, 8), rows_of(start, size, 128)],
            ft.at[:, rows_of(base + start, size, 128)],
            back_s.at[kind, dc], back_r.at[kind, dc], peer(dz, dc),
        )

    short = [back(1, dc, 0, n, quarter - n) for dc in range(2)]
    full = [back(1, dc, 0, 0, quarter) for dc in range(2)]
    even = [back(3, dc, 1, quarter, quarter) for dc in range(2)]
    rest = [[back(3, dc, kind, kind * quarter, quarter) for dc in range(2)] for kind in (2, 3)]
    odd = [back(dz, dc, kind, col * half, half) for dc in range(2) for dz, kind in ((1, 0), (3, 1))]

    def on_kind(step):
        @pl.when(row == 0)
        def _():
            for copy in short + even:
                step(copy)

        @pl.when(row == 1)
        def _():
            for copy in full + even:
                step(copy)

        @pl.when(lo == 1)
        def _():
            for copy in odd:
                step(copy)

    given = []

    def factor_rows(slot, start, size):
        lanes, out = rows_of(start, size, 128), rows_of(base + start, size, 128)
        got = dot3(lefts, split(cr[:, lanes]))
        near[:, lanes] = got[:nh]
        ft[:, out] = got[nh:nh + width]
        own[:, lanes] = got[nh + width:]
        copy = remote(own.at[:, lanes], ft.at[:, out], give_s.at[slot], give_r.at[slot], peer(0, 1))
        copy.start()
        given.append(copy)

    factor_rows(0, early * half, half)
    on_kind(lambda copy: copy.start())

    s_load.wait()
    inverse = split(e[...])
    wh[...] = dot3(inverse, split(s[...]))

    @pl.when(row == 2)
    def _():
        to_first.wait_recv()
        pass_first.start()
        pass_second.wait_recv()

    @pl.when(row == 3)
    def _():
        to_second.wait_recv()
        pass_second.start()
        pass_first.wait_recv()

    @pl.when(row == 1)
    def _():
        to_core.wait_recv()

    y[...] = dot3(inverse, split(vt[...]))
    zv[...] = dot3(split(e[...].T), split(y[...]))

    step = 256

    zs = split(zv[...])

    def project(start, size):
        for i in range(size // step):
            part = rows_of(start + i * step, step, 128)
            pr[part, :] = v[part, :] - dot3(split(cr[:, part].T), zs)

    project(early * half, half)

    for turn in (1, 2):
        late = (1 - early) * half + (turn - 1) * quarter
        for copy in cols[turn]:
            copy.wait_recv()
        factor_rows(turn, late, quarter)

        @pl.when(lo == 0)
        def _():
            for copy in rest[turn - 1]:
                copy.start()

        project(late, quarter)

    @pl.when(row == 0)
    def _():
        to_core.wait_send()
        to_first.wait_send()
        to_second.wait_send()
        pr[pl.ds(0, n), :] = y[...]

    @pl.when(row == 2)
    def _():
        pass_first.wait_send()

    @pl.when(row == 3)
    def _():
        pass_second.wait_send()

    for copy in cols[0] + cols[1] + cols[2]:
        copy.wait_send()
    on_kind(lambda copy: copy.wait_send())

    @pl.when(lo == 0)
    def _():
        for copy in rest[0] + rest[1]:
            copy.wait_send()
        for copy in odd:
            copy.wait_recv()

    @pl.when(lo == 1)
    def _():
        @pl.when(core == 0)
        def _():
            short[0].wait_recv()
            full[1].wait_recv()

        @pl.when(core == 1)
        def _():
            full[0].wait_recv()
            short[1].wait_recv()

        for copy in even + rest[0] + rest[1]:
            copy.wait_recv()

    for copy in given:
        copy.wait()
    ft[:, pl.ds(0, n)] = a[mine, :]


def store(*refs):
    sems = refs[6]
    copies = [pltpu.make_async_copy(refs[i], refs[3 + i], sems.at[i]) for i in range(3)]
    for copy in copies:
        copy.start()
    for copy in copies:
        copy.wait()


def shards(foreground_cols, signal_rows, visibilities):
    length, width = foreground_cols.shape
    n = signal_rows.shape[0]
    span, vecs = visibilities.shape
    vmem = pl.BlockSpec(memory_space=pltpu.VMEM)
    hbm = pl.BlockSpec(memory_space=pl.ANY)
    dma = pltpu.SemaphoreType.DMA
    buffers = (
        (width, length), (n, span), signal_rows.shape, visibilities.shape, (n, vecs), (n, n), (n, n), (n, n),
        (B, B), (B, B), (n, vecs), (n, vecs), (n // 2 + 2 * width, n), (n // 2, span), (width, span),
    )
    ft, whitened, projected = pl.pallas_call(
        kernel,
        name="whiten",
        out_shape=[
            pltpu.VMEM((width, length), F32),
            pltpu.VMEM(signal_rows.shape, F32),
            pltpu.VMEM(visibilities.shape, F32),
        ],
        in_specs=[hbm] * 3,
        out_specs=[vmem] * 3,
        scratch_shapes=[pltpu.VMEM(shape, F32) for shape in buffers]
        + [dma(k) for k in ((5,), (3,), (3,), (4,), (4,), (3, 7), (3, 7), (3,), (2,), (4, 2), (4, 2), (3,), (3,))],
        compiler_params=pltpu.CompilerParams(
            collective_id=0, has_side_effects=True, vmem_limit_bytes=56 * 1024 * 1024
        ),
    )(foreground_cols.T, signal_rows, visibilities)
    ft, whitened, projected = pl.pallas_call(
        store,
        name="store",
        out_shape=[jax.ShapeDtypeStruct(x.shape, F32) for x in (ft, whitened, projected)],
        in_specs=[vmem] * 3,
        out_specs=[hbm] * 3,
        scratch_shapes=[dma((3,))],
        compiler_params=pltpu.CompilerParams(vmem_limit_bytes=1024 * 1024),
    )(ft, whitened, projected)
    return ft.T, whitened, projected


def solution(mesh):
    return jax.shard_map(
        shards,
        mesh=mesh,
        in_specs=(P("ma", ("row", "col")), P("ma", ("row", "col")), P(("ma", "row"), "col")),
        out_specs=(P("ma", ("row", "col")), P("ma", ("row", "col")), P(("ma", "row"), "col")),
        check_vma=False,
    )
```

```python
import jax
import jax.numpy as jnp
from jax import lax
from jax.experimental import pallas as pl
from jax.experimental.pallas import tpu as pltpu
from jax.sharding import PartitionSpec as P

MESH = pl.DeviceIdType.MESH
F32 = jnp.float32
B = 128
HI = lax.Precision.HIGHEST

def dot(a, b, dims=((1,), (0,))):
    return lax.dot_general(a, b, (dims, ((), ())), precision=HI, preferred_element_type=jnp.float32)

def diag_block(d_ref, e_ref):
    for p in range(B // 8):
        c0 = 8 * p
        rows = pl.ds(c0, 8)
        panel = d_ref[rows, :]
        cols = [jnp.broadcast_to(panel[:, c0 + j:c0 + j + 1], (8, B)) for j in range(8)]
        s = {(i, j): jnp.broadcast_to(cols[j][i:i + 1, :], (8, B)) for j in range(8) for i in range(j, 8)}
        w = [jnp.broadcast_to(panel[i:i + 1, :], (8, B)) for i in range(8)]
        ep = e_ref[rows, :]
        v = [jnp.broadcast_to(ep[i:i + 1, :], (8, B)) for i in range(8)]
        r = []
        for j in range(8):
            r.append(lax.rsqrt(s[j, j]))
            for i in range(j + 1, 8):
                s[i, j] = s[i, j] * r[j]
            for k in range(j + 1, 8):
                for i in range(k, 8):
                    s[i, k] = s[i, k] - s[i, j] * s[k, j]
            w[j] = w[j] * r[j]
            v[j] = v[j] * r[j]
            for i in range(j + 1, 8):
                w[i] = w[i] - s[i, j] * w[j]
                v[i] = v[i] - s[i, j] * v[j]
        for j in range(8):
            d_ref[pl.ds(c0 + j, 1), :] = w[j][:1]
            e_ref[pl.ds(c0 + j, 1), :] = v[j][:1]
        for q in range(p + 1, B // 8):
            rq = pl.ds(8 * q, 8)
            dq = d_ref[rq, :]
            eq = e_ref[rq, :]
            g = [jnp.broadcast_to(dq[:, c0 + j:c0 + j + 1], (8, B)) for j in range(8)]
            for j in range(8):
                g[j] = g[j] * r[j]
                for k in range(j + 1, 8):
                    g[k] = g[k] - g[j] * s[k, j]
                dq = dq - g[j] * w[j]
                eq = eq - g[j] * v[j]
            d_ref[rq, :] = dq
            e_ref[rq, :] = eq

def factor(a_ref, e_ref, d_ref, f_ref):
    n = a_ref.shape[0]
    eye = (lax.broadcasted_iota(jnp.int32, (n, n), 0) == lax.broadcasted_iota(jnp.int32, (n, n), 1))
    e_ref[...] = eye.astype(jnp.float32)
    def step(b, _):
        blk = pl.ds(pl.multiple_of(b * B, B), B)
        d_ref[...] = a_ref[blk, blk]
        f_ref[...] = eye[:B, :B].astype(jnp.float32)
        diag_block(d_ref, f_ref)
        inv = f_ref[...]
        below = lax.broadcasted_iota(jnp.int32, (n, B), 0) >= (b + 1) * B
        left = jnp.where(below, dot(a_ref[:, blk], inv, ((1,), (1,))), 0.0)
        top = dot(inv, a_ref[blk, :])
        etop = dot(inv, e_ref[blk, :])
        a_ref[...] = a_ref[...] - dot(left, top)
        e_ref[...] = e_ref[...] - dot(left, etop)
        a_ref[blk, :] = top
        e_ref[blk, :] = etop
        a_ref[blk, blk] = d_ref[...]
        return 0
    lax.fori_loop(0, n // B, step, 0)
    upper = lax.broadcasted_iota(jnp.int32, (n, n), 0) <= lax.broadcasted_iota(jnp.int32, (n, n), 1)
    a_ref[...] = jnp.where(upper, a_ref[...], 0.0)


PEERS = ((1, 0), (3, 0), (2, 0), (1, 1), (3, 1), (2, 1), (0, 1))
FAR = ((1, 0), (3, 0), (2, 0))


def rows_of(start, size, unit):
    return pl.ds(pl.multiple_of(start, unit), size)


def split(x):
    high = x.astype(jnp.bfloat16)
    return high, (x - high.astype(F32)).astype(jnp.bfloat16)


def dot3(a, b):
    def one(x, y):
        return lax.dot_general(x, y, (((1,), (0,)), ((), ())), preferred_element_type=F32)

    return one(a[0], b[0]) + (one(a[0], b[1]) + one(a[1], b[0]))


def kernel(ct_hbm, s_hbm, v_hbm, ft, wh, pr,
           ct, cr, s, v, vt, square, a, e, d, f, y, zv, left, near, own,
           load_sem, top_s, top_r, pass_s, pass_r, col_s, col_r, vec_s, vec_r, back_s, back_r, give_s, give_r):
    width, length = ct.shape
    n = square.shape[0]
    span = v.shape[0]
    half = span // 2
    nh = n // 2
    row, col = lax.axis_index("row"), lax.axis_index("col")
    lo, core = row // 2, row % 2
    z = col * 2 + lo

    def place(dz, dc):
        zz, cc = (z + dz) % 4, (core + dc) % 2
        return (zz % 2) * 2 + cc, zz // 2

    def peer(dz, dc):
        r, c = place(dz, dc)
        return {"row": r, "col": c}

    def band(dz, dc):
        r, c = place(dz, dc)
        return rows_of((r * 2 + c) * width, width, 8)

    def remote(src, dst, send, recv, to):
        return pltpu.make_async_remote_copy(
            src_ref=src, dst_ref=dst, send_sem=send, recv_sem=recv, device_id=to, device_id_type=MESH
        )

    mine = band(0, 0)
    top_load = pltpu.make_async_copy(ct_hbm.at[:, pl.ds(0, n)], square.at[mine, :], load_sem.at[0])
    ct_load = pltpu.make_async_copy(ct_hbm, ct, load_sem.at[1])
    cr_load = pltpu.make_async_copy(
        ct_hbm.at[:, rows_of(row * span, span, 128)], cr.at[mine, :], load_sem.at[2]
    )
    v_load = pltpu.make_async_copy(v_hbm, v, load_sem.at[3])
    s_load = pltpu.make_async_copy(s_hbm, s, load_sem.at[4])
    for load in (top_load, ct_load, cr_load, v_load, s_load):
        load.start()

    barrier = pltpu.get_barrier_semaphore()
    for dz, dc in PEERS:
        pl.semaphore_signal(barrier, inc=1, device_id=peer(dz, dc), device_id_type=MESH)
    pl.semaphore_wait(barrier, len(PEERS))

    top_load.wait()
    def band_sizes(source_lo, step):
        for when, size in ((source_lo == 1, n), (source_lo * 2 + core == 0, B), (source_lo * 2 + core == 1, 2 * B)):
            @pl.when(when)
            def _():
                step(size)

    def top(i, size):
        block = square.at[mine, pl.ds(0, size)]
        return remote(block, block, top_s.at[i], top_r.at[i], peer(*FAR[i]))

    def top_in(i, size):
        block = square.at[band(-FAR[i][0], 0), pl.ds(0, size)]
        return remote(block, block, top_s.at[i], top_r.at[i], peer(*FAR[i]))

    def handed(i, size):
        block = square.at[band(-FAR[i][0] if i < 3 else 0, 0), pl.ds(0, size)]
        return remote(block, block, pass_s.at[i], pass_r.at[i], peer(0, 1))

    def got(i, size):
        block = square.at[band(-FAR[i][0] if i < 3 else 0, 1), pl.ds(0, size)]
        return remote(block, block, pass_s.at[i], pass_r.at[i], peer(0, 1))

    def source(i):
        return (lo + (FAR[i][0] if i < 3 else 0)) % 2

    def start_tops(size):
        for i in range(3):
            top(i, size).start()
        handed(3, size).start()

    band_sizes(lo, start_tops)

    ct_load.wait()
    quarter = half // 2
    cut = quarter + B
    cols = [[], [], []]
    for turn, size in enumerate((half, quarter, quarter)):
        for i, (dz, dc) in enumerate(PEERS):
            r, c = place(dz, dc)
            early = (r // 2) * c
            start = early * half if turn == 0 else (1 - early) * half + (turn - 1) * quarter
            cols[turn].append(remote(
                ct.at[:, rows_of(r * span + start, size, 128)], cr.at[mine, rows_of(start, size, 128)],
                col_s.at[turn, i], col_r.at[turn, i], peer(dz, dc),
            ))
    less = [
        remote(
            ct.at[:, pl.ds(n, half - n)], cr.at[mine, pl.ds(n, half - n)],
            col_s.at[0, i], col_r.at[0, i], peer(dz, dc),
        )
        for i, (dz, dc) in enumerate(PEERS)
    ]

    def first_turn(step):
        for i, (dz, dc) in enumerate(PEERS):
            r, _ = place(dz, dc)

            @pl.when(r == 0)
            def _():
                step(less[i])

            @pl.when(r != 0)
            def _():
                step(cols[0][i])

    first_turn(lambda copy: copy.start())

    v_load.wait()
    first, second = pl.ds(0, nh), pl.ds(nh, nh)
    to_core = remote(v.at[pl.ds(0, n), :], vt, vec_s.at[0], vec_r.at[0], {"row": 1, "col": col})
    to_first = remote(v.at[first, :], vt.at[first, :], vec_s.at[1], vec_r.at[1], {"row": 2, "col": col})
    to_second = remote(v.at[second, :], vt.at[second, :], vec_s.at[2], vec_r.at[1], {"row": 3, "col": col})
    pass_first = remote(vt.at[first, :], vt.at[first, :], vec_s.at[0], vec_r.at[0], {"row": 3, "col": col})
    pass_second = remote(vt.at[second, :], vt.at[second, :], vec_s.at[0], vec_r.at[0], {"row": 2, "col": col})

    @pl.when(row == 0)
    def _():
        to_core.start()
        to_first.start()
        to_second.start()
        vt[...] = v[pl.ds(0, n), :]

    for copy in cols[1] + cols[2]:
        copy.start()

    for i in range(3):
        def forward(size, i=i):
            top_in(i, size).wait_recv()
            handed(i, size).start()

        band_sizes(source(i), forward)

    for i in range(4):
        @pl.when(source(i) == 1)
        def _():
            got(i, n).wait_recv()

        @pl.when((source(i) == 0) & (core == 1))
        def _():
            got(i, B).wait_recv()

        @pl.when((source(i) == 0) & (core == 0))
        def _():
            got(i, 2 * B).wait_recv()

        band_sizes(source(i), lambda size, i=i: handed(i, size).wait_send())

    def end_tops(size):
        for i in range(3):
            top(i, size).wait_send()

    band_sizes(lo, end_tops)
    below = lax.broadcasted_iota(jnp.int32, (n, n), 0) >= lax.broadcasted_iota(jnp.int32, (n, n), 1)
    a[...] = jnp.where(below, square[...], square[...].T)

    cr_load.wait()

    @pl.when(row == 0)
    def _():
        cr[:, pl.ds(0, n)] = a[...]

    factor(a, e, d, f)
    left[pl.ds(0, nh), :] = e[rows_of((1 - lo) * nh, nh, 8), :]
    for j in range(2):
        left[pl.ds(nh + j * width, width), :] = e[band(0, j), :]

    @pl.when(row == 0)
    def _():
        for copy in less:
            copy.wait_recv()

    @pl.when(row != 0)
    def _():
        for copy in cols[0]:
            copy.wait_recv()

    early = lo * col
    base = row * span
    lefts = split(left[...])
    def back(dz, dc, kind, start, size):
        r, c = place(dz, dc)
        return remote(
            near.at[rows_of((r % 2) * 2 * width + c * width, width, 8), rows_of(start, size, 128)],
            ft.at[:, rows_of(base + start, size, 128)],
            back_s.at[kind, dc], back_r.at[kind, dc], peer(dz, dc),
        )

    short = [back(1, dc, 0, n, cut - n) for dc in range(2)]
    full = [back(1, dc, 0, 0, cut) for dc in range(2)]
    even = [back(3, dc, 1, cut, half - cut) for dc in range(2)]
    rest = [[back(3, dc, kind, kind * quarter, quarter) for dc in range(2)] for kind in (2, 3)]
    odd = [back(dz, dc, kind, col * half, half) for dc in range(2) for dz, kind in ((1, 0), (3, 1))]

    def on_kind(step):
        @pl.when(row == 0)
        def _():
            for copy in short + even:
                step(copy)

        @pl.when(row == 1)
        def _():
            for copy in full + even:
                step(copy)

        @pl.when(lo == 1)
        def _():
            for copy in odd:
                step(copy)

    given = []

    def factor_rows(slot, start, size):
        lanes, out = rows_of(start, size, 128), rows_of(base + start, size, 128)
        got = dot3(lefts, split(cr[:, lanes]))
        near[:, lanes] = got[:nh]
        ft[:, out] = got[nh:nh + width]
        own[:, lanes] = got[nh + width:]
        copy = remote(own.at[:, lanes], ft.at[:, out], give_s.at[slot], give_r.at[slot], peer(0, 1))
        copy.start()
        given.append(copy)

    factor_rows(0, early * half, half)
    on_kind(lambda copy: copy.start())

    s_load.wait()
    inverse = split(e[...])
    wh[...] = dot3(inverse, split(s[...]))

    @pl.when(row == 2)
    def _():
        to_first.wait_recv()
        pass_first.start()
        pass_second.wait_recv()

    @pl.when(row == 3)
    def _():
        to_second.wait_recv()
        pass_second.start()
        pass_first.wait_recv()

    @pl.when(row == 1)
    def _():
        to_core.wait_recv()

    y[...] = dot3(inverse, split(vt[...]))
    zv[...] = dot3(split(e[...].T), split(y[...]))

    step = 256

    zs = split(zv[...])

    def project(start, size):
        for i in range(size // step):
            part = rows_of(start + i * step, step, 128)
            pr[part, :] = v[part, :] - dot3(split(cr[:, part].T), zs)

    project(early * half, half)

    for turn in (1, 2):
        late = (1 - early) * half + (turn - 1) * quarter
        for copy in cols[turn]:
            copy.wait_recv()
        factor_rows(turn, late, quarter)

        @pl.when(lo == 0)
        def _():
            for copy in rest[turn - 1]:
                copy.start()

        project(late, quarter)

    @pl.when(row == 0)
    def _():
        to_core.wait_send()
        to_first.wait_send()
        to_second.wait_send()
        pr[pl.ds(0, n), :] = y[...]

    @pl.when(row == 2)
    def _():
        pass_first.wait_send()

    @pl.when(row == 3)
    def _():
        pass_second.wait_send()

    first_turn(lambda copy: copy.wait_send())
    for copy in cols[1] + cols[2]:
        copy.wait_send()
    on_kind(lambda copy: copy.wait_send())

    @pl.when(lo == 0)
    def _():
        for copy in rest[0] + rest[1]:
            copy.wait_send()
        for copy in odd:
            copy.wait_recv()

    @pl.when(lo == 1)
    def _():
        @pl.when(core == 0)
        def _():
            short[0].wait_recv()
            full[1].wait_recv()

        @pl.when(core == 1)
        def _():
            full[0].wait_recv()
            short[1].wait_recv()

        for copy in even + rest[0] + rest[1]:
            copy.wait_recv()

    for copy in given:
        copy.wait()
    ft[:, pl.ds(0, n)] = a[mine, :]


def store(*refs):
    sems = refs[6]
    copies = [pltpu.make_async_copy(refs[i], refs[3 + i], sems.at[i]) for i in range(3)]
    for copy in copies:
        copy.start()
    for copy in copies:
        copy.wait()


def shards(foreground_cols, signal_rows, visibilities):
    length, width = foreground_cols.shape
    n = signal_rows.shape[0]
    span, vecs = visibilities.shape
    vmem = pl.BlockSpec(memory_space=pltpu.VMEM)
    hbm = pl.BlockSpec(memory_space=pl.ANY)
    dma = pltpu.SemaphoreType.DMA
    buffers = (
        (width, length), (n, span), signal_rows.shape, visibilities.shape, (n, vecs), (n, n), (n, n), (n, n),
        (B, B), (B, B), (n, vecs), (n, vecs), (n // 2 + 2 * width, n), (n // 2, span), (width, span),
    )
    ft, whitened, projected = pl.pallas_call(
        kernel,
        name="whiten",
        out_shape=[
            pltpu.VMEM((width, length), F32),
            pltpu.VMEM(signal_rows.shape, F32),
            pltpu.VMEM(visibilities.shape, F32),
        ],
        in_specs=[hbm] * 3,
        out_specs=[vmem] * 3,
        scratch_shapes=[pltpu.VMEM(shape, F32) for shape in buffers]
        + [dma(k) for k in ((5,), (3,), (3,), (4,), (4,), (3, 7), (3, 7), (3,), (2,), (4, 2), (4, 2), (3,), (3,))],
        compiler_params=pltpu.CompilerParams(
            collective_id=0, has_side_effects=True, vmem_limit_bytes=56 * 1024 * 1024
        ),
    )(foreground_cols.T, signal_rows, visibilities)
    ft, whitened, projected = pl.pallas_call(
        store,
        name="store",
        out_shape=[jax.ShapeDtypeStruct(x.shape, F32) for x in (ft, whitened, projected)],
        in_specs=[vmem] * 3,
        out_specs=[hbm] * 3,
        scratch_shapes=[dma((3,))],
        compiler_params=pltpu.CompilerParams(vmem_limit_bytes=1024 * 1024),
    )(ft, whitened, projected)
    return ft.T, whitened, projected


def solution(mesh):
    return jax.shard_map(
        shards,
        mesh=mesh,
        in_specs=(P("ma", ("row", "col")), P("ma", ("row", "col")), P(("ma", "row"), "col")),
        out_specs=(P("ma", ("row", "col")), P("ma", ("row", "col")), P(("ma", "row"), "col")),
        check_vma=False,
    )
```

```python
import jax
import jax.numpy as jnp
from jax import lax
from jax.experimental import pallas as pl
from jax.experimental.pallas import tpu as pltpu
from jax.sharding import PartitionSpec as P

MESH = pl.DeviceIdType.MESH
F32 = jnp.float32
B = 128
HI = lax.Precision.HIGHEST

def dot(a, b, dims=((1,), (0,))):
    return lax.dot_general(a, b, (dims, ((), ())), precision=HI, preferred_element_type=jnp.float32)

def diag_block(d_ref, e_ref):
    for p in range(B // 8):
        c0 = 8 * p
        rows = pl.ds(c0, 8)
        panel = d_ref[rows, :]
        cols = [jnp.broadcast_to(panel[:, c0 + j:c0 + j + 1], (8, B)) for j in range(8)]
        s = {(i, j): jnp.broadcast_to(cols[j][i:i + 1, :], (8, B)) for j in range(8) for i in range(j, 8)}
        w = [jnp.broadcast_to(panel[i:i + 1, :], (8, B)) for i in range(8)]
        ep = e_ref[rows, :]
        v = [jnp.broadcast_to(ep[i:i + 1, :], (8, B)) for i in range(8)]
        r = []
        for j in range(8):
            r.append(lax.rsqrt(s[j, j]))
            for i in range(j + 1, 8):
                s[i, j] = s[i, j] * r[j]
            for k in range(j + 1, 8):
                for i in range(k, 8):
                    s[i, k] = s[i, k] - s[i, j] * s[k, j]
            w[j] = w[j] * r[j]
            v[j] = v[j] * r[j]
            for i in range(j + 1, 8):
                w[i] = w[i] - s[i, j] * w[j]
                v[i] = v[i] - s[i, j] * v[j]
        for j in range(8):
            d_ref[pl.ds(c0 + j, 1), :] = w[j][:1]
            e_ref[pl.ds(c0 + j, 1), :] = v[j][:1]
        for q in range(p + 1, B // 8):
            rq = pl.ds(8 * q, 8)
            dq = d_ref[rq, :]
            eq = e_ref[rq, :]
            g = [jnp.broadcast_to(dq[:, c0 + j:c0 + j + 1], (8, B)) for j in range(8)]
            for j in range(8):
                g[j] = g[j] * r[j]
                for k in range(j + 1, 8):
                    g[k] = g[k] - g[j] * s[k, j]
                dq = dq - g[j] * w[j]
                eq = eq - g[j] * v[j]
            d_ref[rq, :] = dq
            e_ref[rq, :] = eq

def factor(a_ref, e_ref, d_ref, f_ref):
    n = a_ref.shape[0]
    eye = (lax.broadcasted_iota(jnp.int32, (n, n), 0) == lax.broadcasted_iota(jnp.int32, (n, n), 1))
    e_ref[...] = eye.astype(jnp.float32)
    def step(b, _):
        blk = pl.ds(pl.multiple_of(b * B, B), B)
        d_ref[...] = a_ref[blk, blk]
        f_ref[...] = eye[:B, :B].astype(jnp.float32)
        diag_block(d_ref, f_ref)
        inv = f_ref[...]
        below = lax.broadcasted_iota(jnp.int32, (n, B), 0) >= (b + 1) * B
        left = jnp.where(below, dot(a_ref[:, blk], inv, ((1,), (1,))), 0.0)
        top = dot(inv, a_ref[blk, :])
        etop = dot(inv, e_ref[blk, :])
        a_ref[...] = a_ref[...] - dot(left, top)
        e_ref[...] = e_ref[...] - dot(left, etop)
        a_ref[blk, :] = top
        e_ref[blk, :] = etop
        a_ref[blk, blk] = d_ref[...]
        return 0
    lax.fori_loop(0, n // B, step, 0)
    upper = lax.broadcasted_iota(jnp.int32, (n, n), 0) <= lax.broadcasted_iota(jnp.int32, (n, n), 1)
    a_ref[...] = jnp.where(upper, a_ref[...], 0.0)


PEERS = ((1, 0), (3, 0), (2, 0), (1, 1), (3, 1), (2, 1), (0, 1))
FAR = ((1, 0), (3, 0), (2, 0))


def rows_of(start, size, unit):
    return pl.ds(pl.multiple_of(start, unit), size)


def split(x):
    high = x.astype(jnp.bfloat16)
    return high, (x - high.astype(F32)).astype(jnp.bfloat16)


def dot3(a, b):
    def one(x, y):
        return lax.dot_general(x, y, (((1,), (0,)), ((), ())), preferred_element_type=F32)

    return one(a[0], b[0]) + (one(a[0], b[1]) + one(a[1], b[0]))


def kernel(ct_hbm, s_hbm, v_hbm, ft, wh, pr,
           ct, cr, s, v, vt, square, a, e, d, f, y, zv, left, near, own,
           load_sem, top_s, top_r, pass_s, pass_r, col_s, col_r, vec_s, vec_r, back_s, back_r, give_s, give_r):
    width, length = ct.shape
    n = square.shape[0]
    span = v.shape[0]
    half = span // 2
    nh = n // 2
    row, col = lax.axis_index("row"), lax.axis_index("col")
    lo, core = row // 2, row % 2
    z = col * 2 + lo

    def place(dz, dc):
        zz, cc = (z + dz) % 4, (core + dc) % 2
        return (zz % 2) * 2 + cc, zz // 2

    def peer(dz, dc):
        r, c = place(dz, dc)
        return {"row": r, "col": c}

    def band(dz, dc):
        r, c = place(dz, dc)
        return rows_of((r * 2 + c) * width, width, 8)

    def remote(src, dst, send, recv, to):
        return pltpu.make_async_remote_copy(
            src_ref=src, dst_ref=dst, send_sem=send, recv_sem=recv, device_id=to, device_id_type=MESH
        )

    mine = band(0, 0)
    top_load = pltpu.make_async_copy(ct_hbm.at[:, pl.ds(0, n)], square.at[mine, :], load_sem.at[0])
    ct_load = pltpu.make_async_copy(ct_hbm, ct, load_sem.at[1])
    cr_load = pltpu.make_async_copy(
        ct_hbm.at[:, rows_of(row * span, span, 128)], cr.at[mine, :], load_sem.at[2]
    )
    v_load = pltpu.make_async_copy(v_hbm, v, load_sem.at[3])
    s_load = pltpu.make_async_copy(s_hbm, s, load_sem.at[4])
    for load in (top_load, ct_load, cr_load, v_load, s_load):
        load.start()

    barrier = pltpu.get_barrier_semaphore()
    for dz, dc in PEERS:
        pl.semaphore_signal(barrier, inc=1, device_id=peer(dz, dc), device_id_type=MESH)
    pl.semaphore_wait(barrier, len(PEERS))

    top_load.wait()
    def band_sizes(source_lo, step):
        for when, size in ((source_lo == 1, n), (source_lo * 2 + core == 0, B), (source_lo * 2 + core == 1, 2 * B)):
            @pl.when(when)
            def _():
                step(size)

    def top(i, size):
        block = square.at[mine, pl.ds(0, size)]
        return remote(block, block, top_s.at[i], top_r.at[i], peer(*FAR[i]))

    def top_in(i, size):
        block = square.at[band(-FAR[i][0], 0), pl.ds(0, size)]
        return remote(block, block, top_s.at[i], top_r.at[i], peer(*FAR[i]))

    def handed(i, size):
        block = square.at[band(-FAR[i][0] if i < 3 else 0, 0), pl.ds(0, size)]
        return remote(block, block, pass_s.at[i], pass_r.at[i], peer(0, 1))

    def got(i, size):
        block = square.at[band(-FAR[i][0] if i < 3 else 0, 1), pl.ds(0, size)]
        return remote(block, block, pass_s.at[i], pass_r.at[i], peer(0, 1))

    def source(i):
        return (lo + (FAR[i][0] if i < 3 else 0)) % 2

    def start_tops(size):
        for i in range(3):
            top(i, size).start()
        handed(3, size).start()

    band_sizes(lo, start_tops)

    ct_load.wait()
    quarter = half // 2
    cut = quarter + B
    cols = [[], [], []]
    for turn, size in enumerate((half, quarter, quarter)):
        for i, (dz, dc) in enumerate(PEERS):
            r, c = place(dz, dc)
            early = (r // 2) * c
            start = early * half if turn == 0 else (1 - early) * half + (turn - 1) * quarter
            cols[turn].append(remote(
                ct.at[:, rows_of(r * span + start, size, 128)], cr.at[mine, rows_of(start, size, 128)],
                col_s.at[turn, i], col_r.at[turn, i], peer(dz, dc),
            ))
    less = [
        remote(
            ct.at[:, pl.ds(n, half - n)], cr.at[mine, pl.ds(n, half - n)],
            col_s.at[0, i], col_r.at[0, i], peer(dz, dc),
        )
        for i, (dz, dc) in enumerate(PEERS)
    ]

    def first_turn(step):
        for i, (dz, dc) in enumerate(PEERS):
            r, _ = place(dz, dc)

            @pl.when(r == 0)
            def _():
                step(less[i])

            @pl.when(r != 0)
            def _():
                step(cols[0][i])


    v_load.wait()
    first, second = pl.ds(0, nh), pl.ds(nh, nh)
    to_core = remote(v.at[pl.ds(0, n), :], vt, vec_s.at[0], vec_r.at[0], {"row": 1, "col": col})
    to_first = remote(v.at[first, :], vt.at[first, :], vec_s.at[1], vec_r.at[1], {"row": 2, "col": col})
    to_second = remote(vt.at[second, :], vt.at[second, :], vec_s.at[1], vec_r.at[1], {"row": 3, "col": col})
    pass_first = remote(vt.at[first, :], vt.at[first, :], vec_s.at[0], vec_r.at[0], {"row": 3, "col": col})
    pass_second = remote(vt.at[second, :], vt.at[second, :], vec_s.at[0], vec_r.at[0], {"row": 2, "col": col})

    @pl.when(row == 0)
    def _():
        to_core.start()
        to_first.start()
        vt[...] = v[pl.ds(0, n), :]

    @pl.when(row == 1)
    def _():
        to_core.wait_recv()
        to_second.start()

    first_turn(lambda copy: copy.start())
    same = [i for i, (dz, _) in enumerate(PEERS) if dz % 2 == 0]
    apart = [i for i, (dz, _) in enumerate(PEERS) if dz % 2 == 1]
    for own_lo, order in ((0, (same, apart)), (1, (apart, same))):
        @pl.when(lo == own_lo)
        def _():
            for group in order:
                for turn in (1, 2):
                    for i in group:
                        cols[turn][i].start()

    for i in range(3):
        def forward(size, i=i):
            top_in(i, size).wait_recv()
            handed(i, size).start()

        band_sizes(source(i), forward)

    for i in range(4):
        @pl.when(source(i) == 1)
        def _():
            got(i, n).wait_recv()

        @pl.when((source(i) == 0) & (core == 1))
        def _():
            got(i, B).wait_recv()

        @pl.when((source(i) == 0) & (core == 0))
        def _():
            got(i, 2 * B).wait_recv()

        band_sizes(source(i), lambda size, i=i: handed(i, size).wait_send())

    def end_tops(size):
        for i in range(3):
            top(i, size).wait_send()

    band_sizes(lo, end_tops)
    below = lax.broadcasted_iota(jnp.int32, (n, n), 0) >= lax.broadcasted_iota(jnp.int32, (n, n), 1)
    a[...] = jnp.where(below, square[...], square[...].T)

    cr_load.wait()

    @pl.when(row == 0)
    def _():
        cr[:, pl.ds(0, n)] = a[...]

    factor(a, e, d, f)

    @pl.when(row == 2)
    def _():
        to_first.wait_recv()
        pass_first.start()

    @pl.when(row == 3)
    def _():
        to_second.wait_recv()
        pass_second.start()

    s_load.wait()
    inverse = split(e[...])
    wh[...] = dot3(inverse, split(s[...]))

    @pl.when(row == 2)
    def _():
        pass_second.wait_recv()

    @pl.when(row == 3)
    def _():
        pass_first.wait_recv()

    y[...] = dot3(inverse, split(vt[...]))
    zv[...] = dot3(split(e[...].T), split(y[...]))

    left[pl.ds(0, nh), :] = e[rows_of((1 - lo) * nh, nh, 8), :]
    for j in range(2):
        left[pl.ds(nh + j * width, width), :] = e[band(0, j), :]

    @pl.when(row == 0)
    def _():
        for copy in less:
            copy.wait_recv()

    @pl.when(row != 0)
    def _():
        for copy in cols[0]:
            copy.wait_recv()

    early = lo * col
    base = row * span
    lefts = split(left[...])
    def back(dz, dc, kind, start, size):
        r, c = place(dz, dc)
        return remote(
            near.at[rows_of((r % 2) * 2 * width + c * width, width, 8), rows_of(start, size, 128)],
            ft.at[:, rows_of(base + start, size, 128)],
            back_s.at[kind, dc], back_r.at[kind, dc], peer(dz, dc),
        )

    short = [back(1, dc, 0, n, cut - n) for dc in range(2)]
    full = [back(1, dc, 0, 0, cut) for dc in range(2)]
    even = [back(3, dc, 1, cut, half - cut) for dc in range(2)]
    rest = [[back(3, dc, kind, kind * quarter, quarter) for dc in range(2)] for kind in (2, 3)]
    odd = [back(dz, dc, kind, col * half, half) for dc in range(2) for dz, kind in ((1, 0), (3, 1))]

    def on_kind(step):
        @pl.when(row == 0)
        def _():
            for copy in short + even:
                step(copy)

        @pl.when(row == 1)
        def _():
            for copy in full + even:
                step(copy)

        @pl.when(lo == 1)
        def _():
            for copy in odd:
                step(copy)

    def given(slot, start, size):
        out = ft.at[:, rows_of(base + start, size, 128)]
        return remote(own.at[:, rows_of(start, size, 128)], out, give_s.at[slot], give_r.at[slot], peer(0, 1))

    def factor_rows(slot, start, size):
        lanes, out = rows_of(start, size, 128), rows_of(base + start, size, 128)
        got = dot3(lefts, split(cr[:, lanes]))
        near[:, lanes] = got[:nh]
        ft[:, out] = got[nh:nh + width]
        own[:, lanes] = got[nh + width:]
        given(slot, start, size).start()

    factor_rows(0, early * half, half)
    on_kind(lambda copy: copy.start())

    step = 256

    zs = split(zv[...])

    def project(start, size):
        def one(i, _):
            part = rows_of(start + i * step, step, 128)
            pr[part, :] = v[part, :] - dot3(split(cr[:, part].T), zs)
            return 0

        lax.fori_loop(0, size // step, one, 0)

    def late(turn):
        return (1 - early) * half + (turn - 1) * quarter

    @pl.when(lo == 0)
    def _():
        for turn in (1, 2):
            for copy in cols[turn]:
                copy.wait_recv()
            factor_rows(turn, late(turn), quarter)
            for copy in rest[turn - 1]:
                copy.start()
        project(0, span)

    @pl.when(lo == 1)
    def _():
        project(early * half, half)
        for turn in (1, 2):
            for copy in cols[turn]:
                copy.wait_recv()
            factor_rows(turn, late(turn), quarter)
            project(late(turn), quarter)

    @pl.when(row == 0)
    def _():
        to_core.wait_send()
        to_first.wait_send()
        pr[pl.ds(0, n), :] = y[...]

    @pl.when(row == 1)
    def _():
        to_second.wait_send()

    @pl.when(row == 2)
    def _():
        pass_first.wait_send()

    @pl.when(row == 3)
    def _():
        pass_second.wait_send()

    first_turn(lambda copy: copy.wait_send())
    for copy in cols[1] + cols[2]:
        copy.wait_send()
    on_kind(lambda copy: copy.wait_send())

    @pl.when(lo == 0)
    def _():
        for copy in rest[0] + rest[1]:
            copy.wait_send()
        for copy in odd:
            copy.wait_recv()

    @pl.when(lo == 1)
    def _():
        @pl.when(core == 0)
        def _():
            short[0].wait_recv()
            full[1].wait_recv()

        @pl.when(core == 1)
        def _():
            full[0].wait_recv()
            short[1].wait_recv()

        for copy in even + rest[0] + rest[1]:
            copy.wait_recv()

    given(0, early * half, half).wait()
    for turn in (1, 2):
        given(turn, late(turn), quarter).wait()
    ft[:, pl.ds(0, n)] = a[mine, :]


def store(*refs):
    sems = refs[6]
    copies = [pltpu.make_async_copy(refs[i], refs[3 + i], sems.at[i]) for i in range(3)]
    for copy in copies:
        copy.start()
    for copy in copies:
        copy.wait()


def shards(foreground_cols, signal_rows, visibilities):
    length, width = foreground_cols.shape
    n = signal_rows.shape[0]
    span, vecs = visibilities.shape
    vmem = pl.BlockSpec(memory_space=pltpu.VMEM)
    hbm = pl.BlockSpec(memory_space=pl.ANY)
    dma = pltpu.SemaphoreType.DMA
    buffers = (
        (width, length), (n, span), signal_rows.shape, visibilities.shape, (n, vecs), (n, n), (n, n), (n, n),
        (B, B), (B, B), (n, vecs), (n, vecs), (n // 2 + 2 * width, n), (n // 2, span), (width, span),
    )
    ft, whitened, projected = pl.pallas_call(
        kernel,
        name="whiten",
        out_shape=[
            pltpu.VMEM((width, length), F32),
            pltpu.VMEM(signal_rows.shape, F32),
            pltpu.VMEM(visibilities.shape, F32),
        ],
        in_specs=[hbm] * 3,
        out_specs=[vmem] * 3,
        scratch_shapes=[pltpu.VMEM(shape, F32) for shape in buffers]
        + [dma(k) for k in ((5,), (3,), (3,), (4,), (4,), (3, 7), (3, 7), (3,), (2,), (4, 2), (4, 2), (3,), (3,))],
        compiler_params=pltpu.CompilerParams(
            collective_id=0, has_side_effects=True, vmem_limit_bytes=56 * 1024 * 1024
        ),
    )(foreground_cols.T, signal_rows, visibilities)
    ft, whitened, projected = pl.pallas_call(
        store,
        name="store",
        out_shape=[jax.ShapeDtypeStruct(x.shape, F32) for x in (ft, whitened, projected)],
        in_specs=[vmem] * 3,
        out_specs=[hbm] * 3,
        scratch_shapes=[dma((3,))],
        compiler_params=pltpu.CompilerParams(vmem_limit_bytes=1024 * 1024),
    )(ft, whitened, projected)
    return ft.T, whitened, projected


def solution(mesh):
    return jax.shard_map(
        shards,
        mesh=mesh,
        in_specs=(P("ma", ("row", "col")), P("ma", ("row", "col")), P(("ma", "row"), "col")),
        out_specs=(P("ma", ("row", "col")), P("ma", ("row", "col")), P(("ma", "row"), "col")),
        check_vma=False,
    )
```

```python
import jax
import jax.numpy as jnp
from jax import lax
from jax.experimental import pallas as pl
from jax.experimental.pallas import tpu as pltpu
from jax.sharding import PartitionSpec as P

MESH = pl.DeviceIdType.MESH
F32 = jnp.float32
B = 128
HI = lax.Precision.HIGHEST

def dot(a, b, dims=((1,), (0,))):
    return lax.dot_general(a, b, (dims, ((), ())), precision=HI, preferred_element_type=jnp.float32)

def diag_block(d_ref, e_ref):
    for p in range(B // 8):
        c0 = 8 * p
        rows = pl.ds(c0, 8)
        panel = d_ref[rows, :]
        cols = [jnp.broadcast_to(panel[:, c0 + j:c0 + j + 1], (8, B)) for j in range(8)]
        s = {(i, j): jnp.broadcast_to(cols[j][i:i + 1, :], (8, B)) for j in range(8) for i in range(j, 8)}
        w = [jnp.broadcast_to(panel[i:i + 1, :], (8, B)) for i in range(8)]
        ep = e_ref[rows, :]
        v = [jnp.broadcast_to(ep[i:i + 1, :], (8, B)) for i in range(8)]
        r = []
        for j in range(8):
            r.append(lax.rsqrt(s[j, j]))
            for i in range(j + 1, 8):
                s[i, j] = s[i, j] * r[j]
            for k in range(j + 1, 8):
                for i in range(k, 8):
                    s[i, k] = s[i, k] - s[i, j] * s[k, j]
            w[j] = w[j] * r[j]
            v[j] = v[j] * r[j]
            for i in range(j + 1, 8):
                w[i] = w[i] - s[i, j] * w[j]
                v[i] = v[i] - s[i, j] * v[j]
        for j in range(8):
            d_ref[pl.ds(c0 + j, 1), :] = w[j][:1]
            e_ref[pl.ds(c0 + j, 1), :] = v[j][:1]
        for q in range(p + 1, B // 8):
            rq = pl.ds(8 * q, 8)
            dq = d_ref[rq, :]
            eq = e_ref[rq, :]
            g = [jnp.broadcast_to(dq[:, c0 + j:c0 + j + 1], (8, B)) for j in range(8)]
            for j in range(8):
                g[j] = g[j] * r[j]
                for k in range(j + 1, 8):
                    g[k] = g[k] - g[j] * s[k, j]
                dq = dq - g[j] * w[j]
                eq = eq - g[j] * v[j]
            d_ref[rq, :] = dq
            e_ref[rq, :] = eq

def factor(a_ref, e_ref, d_ref, f_ref):
    n = a_ref.shape[0]
    eye = (lax.broadcasted_iota(jnp.int32, (n, n), 0) == lax.broadcasted_iota(jnp.int32, (n, n), 1))
    e_ref[...] = eye.astype(jnp.float32)
    def step(b, _):
        blk = pl.ds(pl.multiple_of(b * B, B), B)
        d_ref[...] = a_ref[blk, blk]
        f_ref[...] = eye[:B, :B].astype(jnp.float32)
        diag_block(d_ref, f_ref)
        inv = f_ref[...]
        below = lax.broadcasted_iota(jnp.int32, (n, B), 0) >= (b + 1) * B
        left = jnp.where(below, dot(a_ref[:, blk], inv, ((1,), (1,))), 0.0)
        top = dot(inv, a_ref[blk, :])
        etop = dot(inv, e_ref[blk, :])
        a_ref[...] = a_ref[...] - dot(left, top)
        e_ref[...] = e_ref[...] - dot(left, etop)
        a_ref[blk, :] = top
        e_ref[blk, :] = etop
        a_ref[blk, blk] = d_ref[...]
        return 0
    lax.fori_loop(0, n // B, step, 0)
    upper = lax.broadcasted_iota(jnp.int32, (n, n), 0) <= lax.broadcasted_iota(jnp.int32, (n, n), 1)
    a_ref[...] = jnp.where(upper, a_ref[...], 0.0)


PEERS = ((1, 0), (3, 0), (2, 0), (1, 1), (3, 1), (2, 1), (0, 1))
FAR = ((1, 0), (3, 0), (2, 0))


def rows_of(start, size, unit):
    return pl.ds(pl.multiple_of(start, unit), size)


def split(x):
    high = x.astype(jnp.bfloat16)
    return high, (x - high.astype(F32)).astype(jnp.bfloat16)


def dot3(a, b):
    def one(x, y):
        return lax.dot_general(x, y, (((1,), (0,)), ((), ())), preferred_element_type=F32)

    return one(a[0], b[0]) + (one(a[0], b[1]) + one(a[1], b[0]))


def kernel(ct_hbm, s_hbm, v_hbm, ft, wh, pr,
           ct, cr, s, v, vt, square, a, e, d, f, y, zv, left, near, own,
           load_sem, top_s, top_r, pass_s, pass_r, col_s, col_r, vec_s, vec_r, back_s, back_r, give_s, give_r):
    width, length = ct.shape
    n = square.shape[0]
    span = v.shape[0]
    half = span // 2
    nh = n // 2
    row, col = lax.axis_index("row"), lax.axis_index("col")
    lo, core = row // 2, row % 2
    z = col * 2 + lo

    def place(dz, dc):
        zz, cc = (z + dz) % 4, (core + dc) % 2
        return (zz % 2) * 2 + cc, zz // 2

    def peer(dz, dc):
        r, c = place(dz, dc)
        return {"row": r, "col": c}

    def band(dz, dc):
        r, c = place(dz, dc)
        return rows_of((r * 2 + c) * width, width, 8)

    def remote(src, dst, send, recv, to):
        return pltpu.make_async_remote_copy(
            src_ref=src, dst_ref=dst, send_sem=send, recv_sem=recv, device_id=to, device_id_type=MESH
        )

    mine = band(0, 0)
    top_load = pltpu.make_async_copy(ct_hbm.at[:, pl.ds(0, n)], square.at[mine, :], load_sem.at[0])
    ct_load = pltpu.make_async_copy(ct_hbm, ct, load_sem.at[1])
    cr_load = pltpu.make_async_copy(
        ct_hbm.at[:, rows_of(row * span, span, 128)], cr.at[mine, :], load_sem.at[2]
    )
    v_load = pltpu.make_async_copy(v_hbm, v, load_sem.at[3])
    s_load = pltpu.make_async_copy(s_hbm, s, load_sem.at[4])
    for load in (top_load, ct_load, cr_load, v_load, s_load):
        load.start()

    barrier = pltpu.get_barrier_semaphore()
    for dz, dc in PEERS:
        pl.semaphore_signal(barrier, inc=1, device_id=peer(dz, dc), device_id_type=MESH)
    pl.semaphore_wait(barrier, len(PEERS))

    top_load.wait()
    def band_sizes(source_lo, step):
        for when, size in ((source_lo == 1, n), (source_lo * 2 + core == 0, B), (source_lo * 2 + core == 1, 2 * B)):
            @pl.when(when)
            def _():
                step(size)

    def top(i, size):
        block = square.at[mine, pl.ds(0, size)]
        return remote(block, block, top_s.at[i], top_r.at[i], peer(*FAR[i]))

    def top_in(i, size):
        block = square.at[band(-FAR[i][0], 0), pl.ds(0, size)]
        return remote(block, block, top_s.at[i], top_r.at[i], peer(*FAR[i]))

    def handed(i, size):
        block = square.at[band(-FAR[i][0] if i < 3 else 0, 0), pl.ds(0, size)]
        return remote(block, block, pass_s.at[i], pass_r.at[i], peer(0, 1))

    def got(i, size):
        block = square.at[band(-FAR[i][0] if i < 3 else 0, 1), pl.ds(0, size)]
        return remote(block, block, pass_s.at[i], pass_r.at[i], peer(0, 1))

    def source(i):
        return (lo + (FAR[i][0] if i < 3 else 0)) % 2

    def start_tops(size):
        for i in range(3):
            top(i, size).start()
        handed(3, size).start()

    band_sizes(lo, start_tops)

    ct_load.wait()
    quarter = half // 2
    cut = quarter + 2 * B
    cols = [[], [], []]
    for turn, size in enumerate((half, quarter, quarter)):
        for i, (dz, dc) in enumerate(PEERS):
            r, c = place(dz, dc)
            early = (r // 2) * c
            start = early * half if turn == 0 else (1 - early) * half + (turn - 1) * quarter
            cols[turn].append(remote(
                ct.at[:, rows_of(r * span + start, size, 128)], cr.at[mine, rows_of(start, size, 128)],
                col_s.at[turn, i], col_r.at[turn, i], peer(dz, dc),
            ))
    less = [
        remote(
            ct.at[:, pl.ds(n, half - n)], cr.at[mine, pl.ds(n, half - n)],
            col_s.at[0, i], col_r.at[0, i], peer(dz, dc),
        )
        for i, (dz, dc) in enumerate(PEERS)
    ]

    def first_turn(step):
        for i, (dz, dc) in enumerate(PEERS):
            r, _ = place(dz, dc)

            @pl.when(r == 0)
            def _():
                step(less[i])

            @pl.when(r != 0)
            def _():
                step(cols[0][i])


    v_load.wait()
    first, second = pl.ds(0, nh), pl.ds(nh, nh)
    to_core = remote(v.at[pl.ds(0, n), :], vt, vec_s.at[0], vec_r.at[0], {"row": 1, "col": col})
    to_first = remote(v.at[first, :], vt.at[first, :], vec_s.at[1], vec_r.at[1], {"row": 2, "col": col})
    to_second = remote(vt.at[second, :], vt.at[second, :], vec_s.at[1], vec_r.at[1], {"row": 3, "col": col})
    pass_first = remote(vt.at[first, :], vt.at[first, :], vec_s.at[0], vec_r.at[0], {"row": 3, "col": col})
    pass_second = remote(vt.at[second, :], vt.at[second, :], vec_s.at[0], vec_r.at[0], {"row": 2, "col": col})

    @pl.when(row == 0)
    def _():
        to_core.start()
        to_first.start()
        vt[...] = v[pl.ds(0, n), :]

    @pl.when(row == 1)
    def _():
        to_core.wait_recv()
        to_second.start()

    first_turn(lambda copy: copy.start())
    same = [i for i, (dz, _) in enumerate(PEERS) if dz % 2 == 0]
    apart = [i for i, (dz, _) in enumerate(PEERS) if dz % 2 == 1]
    for own_lo, order in ((0, (same, apart)), (1, (apart, same))):
        @pl.when(lo == own_lo)
        def _():
            for group in order:
                for turn in (1, 2):
                    for i in group:
                        cols[turn][i].start()

    for i in range(3):
        def forward(size, i=i):
            top_in(i, size).wait_recv()
            handed(i, size).start()

        band_sizes(source(i), forward)

    for i in range(4):
        @pl.when(source(i) == 1)
        def _():
            got(i, n).wait_recv()

        @pl.when((source(i) == 0) & (core == 1))
        def _():
            got(i, B).wait_recv()

        @pl.when((source(i) == 0) & (core == 0))
        def _():
            got(i, 2 * B).wait_recv()

        band_sizes(source(i), lambda size, i=i: handed(i, size).wait_send())

    def end_tops(size):
        for i in range(3):
            top(i, size).wait_send()

    band_sizes(lo, end_tops)
    below = lax.broadcasted_iota(jnp.int32, (n, n), 0) >= lax.broadcasted_iota(jnp.int32, (n, n), 1)
    a[...] = jnp.where(below, square[...], square[...].T)

    cr_load.wait()

    @pl.when(row == 0)
    def _():
        cr[:, pl.ds(0, n)] = a[...]

    factor(a, e, d, f)

    @pl.when(row == 2)
    def _():
        to_first.wait_recv()
        pass_first.start()

    @pl.when(row == 3)
    def _():
        to_second.wait_recv()
        pass_second.start()

    s_load.wait()
    inverse = split(e[...])
    wh[...] = dot3(inverse, split(s[...]))

    @pl.when(row == 2)
    def _():
        pass_second.wait_recv()

    @pl.when(row == 3)
    def _():
        pass_first.wait_recv()

    y[...] = dot3(inverse, split(vt[...]))
    zv[...] = dot3(split(e[...].T), split(y[...]))

    left[pl.ds(0, nh), :] = e[rows_of((1 - lo) * nh, nh, 8), :]
    for j in range(2):
        left[pl.ds(nh + j * width, width), :] = e[band(0, j), :]

    @pl.when(row == 0)
    def _():
        for copy in less:
            copy.wait_recv()

    @pl.when(row != 0)
    def _():
        for copy in cols[0]:
            copy.wait_recv()

    early = lo * col
    base = row * span
    lefts = split(left[...])
    def back(dz, dc, kind, start, size):
        r, c = place(dz, dc)
        return remote(
            near.at[rows_of((r % 2) * 2 * width + c * width, width, 8), rows_of(start, size, 128)],
            ft.at[:, rows_of(base + start, size, 128)],
            back_s.at[kind, dc], back_r.at[kind, dc], peer(dz, dc),
        )

    short = [back(1, dc, 0, n, cut - n) for dc in range(2)]
    full = [back(1, dc, 0, 0, cut) for dc in range(2)]
    even = [back(3, dc, 1, cut, half - cut) for dc in range(2)]
    rest = [[back(3, dc, kind, kind * quarter, quarter) for dc in range(2)] for kind in (2, 3)]
    odd = [back(dz, dc, kind, col * half, half) for dc in range(2) for dz, kind in ((1, 0), (3, 1))]

    def on_kind(step):
        @pl.when(row == 0)
        def _():
            for copy in short + even:
                step(copy)

        @pl.when(row == 1)
        def _():
            for copy in full + even:
                step(copy)

        @pl.when(lo == 1)
        def _():
            for copy in odd:
                step(copy)

    def given(slot, start, size):
        out = ft.at[:, rows_of(base + start, size, 128)]
        return remote(own.at[:, rows_of(start, size, 128)], out, give_s.at[slot], give_r.at[slot], peer(0, 1))

    def factor_rows(slot, start, size):
        lanes, out = rows_of(start, size, 128), rows_of(base + start, size, 128)
        got = dot3(lefts, split(cr[:, lanes]))
        near[:, lanes] = got[:nh]
        ft[:, out] = got[nh:nh + width]
        own[:, lanes] = got[nh + width:]
        given(slot, start, size).start()

    factor_rows(0, early * half, half)
    on_kind(lambda copy: copy.start())

    step = 256

    zs = split(zv[...])

    def project(start, size):
        def one(i, _):
            part = rows_of(start + i * step, step, 128)
            pr[part, :] = v[part, :] - dot3(split(cr[:, part].T), zs)
            return 0

        lax.fori_loop(0, size // step, one, 0)

    def late(turn):
        return (1 - early) * half + (turn - 1) * quarter

    @pl.when(lo == 0)
    def _():
        for turn in (1, 2):
            for copy in cols[turn]:
                copy.wait_recv()
            factor_rows(turn, late(turn), quarter)
            for copy in rest[turn - 1]:
                copy.start()
        project(0, span)

    @pl.when(lo == 1)
    def _():
        project(early * half, half)
        for turn in (1, 2):
            for copy in cols[turn]:
                copy.wait_recv()
            factor_rows(turn, late(turn), quarter)
            project(late(turn), quarter)

    @pl.when(row == 0)
    def _():
        to_core.wait_send()
        to_first.wait_send()
        pr[pl.ds(0, n), :] = y[...]

    @pl.when(row == 1)
    def _():
        to_second.wait_send()

    @pl.when(row == 2)
    def _():
        pass_first.wait_send()

    @pl.when(row == 3)
    def _():
        pass_second.wait_send()

    first_turn(lambda copy: copy.wait_send())
    for copy in cols[1] + cols[2]:
        copy.wait_send()
    on_kind(lambda copy: copy.wait_send())

    @pl.when(lo == 0)
    def _():
        for copy in rest[0] + rest[1]:
            copy.wait_send()
        for copy in odd:
            copy.wait_recv()

    @pl.when(lo == 1)
    def _():
        @pl.when(core == 0)
        def _():
            short[0].wait_recv()
            full[1].wait_recv()

        @pl.when(core == 1)
        def _():
            full[0].wait_recv()
            short[1].wait_recv()

        for copy in even + rest[0] + rest[1]:
            copy.wait_recv()

    given(0, early * half, half).wait()
    for turn in (1, 2):
        given(turn, late(turn), quarter).wait()
    ft[:, pl.ds(0, n)] = a[mine, :]


def store(*refs):
    sems = refs[6]
    copies = [pltpu.make_async_copy(refs[i], refs[3 + i], sems.at[i]) for i in range(3)]
    for copy in copies:
        copy.start()
    for copy in copies:
        copy.wait()


def shards(foreground_cols, signal_rows, visibilities):
    length, width = foreground_cols.shape
    n = signal_rows.shape[0]
    span, vecs = visibilities.shape
    vmem = pl.BlockSpec(memory_space=pltpu.VMEM)
    hbm = pl.BlockSpec(memory_space=pl.ANY)
    dma = pltpu.SemaphoreType.DMA
    buffers = (
        (width, length), (n, span), signal_rows.shape, visibilities.shape, (n, vecs), (n, n), (n, n), (n, n),
        (B, B), (B, B), (n, vecs), (n, vecs), (n // 2 + 2 * width, n), (n // 2, span), (width, span),
    )
    ft, whitened, projected = pl.pallas_call(
        kernel,
        name="whiten",
        out_shape=[
            pltpu.VMEM((width, length), F32),
            pltpu.VMEM(signal_rows.shape, F32),
            pltpu.VMEM(visibilities.shape, F32),
        ],
        in_specs=[hbm] * 3,
        out_specs=[vmem] * 3,
        scratch_shapes=[pltpu.VMEM(shape, F32) for shape in buffers]
        + [dma(k) for k in ((5,), (3,), (3,), (4,), (4,), (3, 7), (3, 7), (3,), (2,), (4, 2), (4, 2), (3,), (3,))],
        compiler_params=pltpu.CompilerParams(
            collective_id=0, has_side_effects=True, vmem_limit_bytes=56 * 1024 * 1024
        ),
    )(foreground_cols.T, signal_rows, visibilities)
    ft, whitened, projected = pl.pallas_call(
        store,
        name="store",
        out_shape=[jax.ShapeDtypeStruct(x.shape, F32) for x in (ft, whitened, projected)],
        in_specs=[vmem] * 3,
        out_specs=[hbm] * 3,
        scratch_shapes=[dma((3,))],
        compiler_params=pltpu.CompilerParams(vmem_limit_bytes=1024 * 1024),
    )(ft, whitened, projected)
    return ft.T, whitened, projected


def solution(mesh):
    return jax.shard_map(
        shards,
        mesh=mesh,
        in_specs=(P("ma", ("row", "col")), P("ma", ("row", "col")), P(("ma", "row"), "col")),
        out_specs=(P("ma", ("row", "col")), P("ma", ("row", "col")), P(("ma", "row"), "col")),
        check_vma=False,
    )
```

```python
import jax
import jax.numpy as jnp
from jax import lax
from jax.experimental import pallas as pl
from jax.experimental.pallas import tpu as pltpu
from jax.sharding import PartitionSpec as P

MESH = pl.DeviceIdType.MESH
F32 = jnp.float32
B = 128
HI = lax.Precision.HIGHEST

def dot(a, b, dims=((1,), (0,))):
    return lax.dot_general(a, b, (dims, ((), ())), precision=HI, preferred_element_type=jnp.float32)

def diag_block(d_ref, e_ref):
    for p in range(B // 8):
        c0 = 8 * p
        rows = pl.ds(c0, 8)
        panel = d_ref[rows, :]
        cols = [jnp.broadcast_to(panel[:, c0 + j:c0 + j + 1], (8, B)) for j in range(8)]
        s = {(i, j): jnp.broadcast_to(cols[j][i:i + 1, :], (8, B)) for j in range(8) for i in range(j, 8)}
        w = [jnp.broadcast_to(panel[i:i + 1, :], (8, B)) for i in range(8)]
        ep = e_ref[rows, :]
        v = [jnp.broadcast_to(ep[i:i + 1, :], (8, B)) for i in range(8)]
        r = []
        for j in range(8):
            r.append(lax.rsqrt(s[j, j]))
            for i in range(j + 1, 8):
                s[i, j] = s[i, j] * r[j]
            for k in range(j + 1, 8):
                for i in range(k, 8):
                    s[i, k] = s[i, k] - s[i, j] * s[k, j]
            w[j] = w[j] * r[j]
            v[j] = v[j] * r[j]
            for i in range(j + 1, 8):
                w[i] = w[i] - s[i, j] * w[j]
                v[i] = v[i] - s[i, j] * v[j]
        for j in range(8):
            d_ref[pl.ds(c0 + j, 1), :] = w[j][:1]
            e_ref[pl.ds(c0 + j, 1), :] = v[j][:1]
        for q in range(p + 1, B // 8):
            rq = pl.ds(8 * q, 8)
            dq = d_ref[rq, :]
            eq = e_ref[rq, :]
            g = [jnp.broadcast_to(dq[:, c0 + j:c0 + j + 1], (8, B)) for j in range(8)]
            for j in range(8):
                g[j] = g[j] * r[j]
                for k in range(j + 1, 8):
                    g[k] = g[k] - g[j] * s[k, j]
                dq = dq - g[j] * w[j]
                eq = eq - g[j] * v[j]
            d_ref[rq, :] = dq
            e_ref[rq, :] = eq

def factor(a_ref, e_ref, d_ref, f_ref):
    n = a_ref.shape[0]
    eye = (lax.broadcasted_iota(jnp.int32, (n, n), 0) == lax.broadcasted_iota(jnp.int32, (n, n), 1))
    e_ref[...] = eye.astype(jnp.float32)
    def step(b, _):
        blk = pl.ds(pl.multiple_of(b * B, B), B)
        d_ref[...] = a_ref[blk, blk]
        f_ref[...] = eye[:B, :B].astype(jnp.float32)
        diag_block(d_ref, f_ref)
        inv = f_ref[...]
        below = lax.broadcasted_iota(jnp.int32, (n, B), 0) >= (b + 1) * B
        left = jnp.where(below, dot(a_ref[:, blk], inv, ((1,), (1,))), 0.0)
        top = dot(inv, a_ref[blk, :])
        etop = dot(inv, e_ref[blk, :])
        a_ref[...] = a_ref[...] - dot(left, top)
        e_ref[...] = e_ref[...] - dot(left, etop)
        a_ref[blk, :] = top
        e_ref[blk, :] = etop
        a_ref[blk, blk] = d_ref[...]
        return 0
    lax.fori_loop(0, n // B, step, 0)
    upper = lax.broadcasted_iota(jnp.int32, (n, n), 0) <= lax.broadcasted_iota(jnp.int32, (n, n), 1)
    a_ref[...] = jnp.where(upper, a_ref[...], 0.0)


PEERS = ((1, 0), (3, 0), (2, 0), (1, 1), (3, 1), (2, 1), (0, 1))
FAR = ((1, 0), (3, 0), (2, 0))


def rows_of(start, size, unit):
    return pl.ds(pl.multiple_of(start, unit), size)


def split(x):
    high = x.astype(jnp.bfloat16)
    return high, (x - high.astype(F32)).astype(jnp.bfloat16)


def dot3(a, b):
    def one(x, y):
        return lax.dot_general(x, y, (((1,), (0,)), ((), ())), preferred_element_type=F32)

    return one(a[0], b[0]) + (one(a[0], b[1]) + one(a[1], b[0]))


def kernel(ct_hbm, s_hbm, v_hbm, ft, wh, pr,
           ct, cr, s, v, vt, square, a, e, d, f, y, zv, left, near, own,
           load_sem, top_s, top_r, pass_s, pass_r, col_s, col_r, vec_s, vec_r, back_s, back_r, give_s, give_r):
    width, length = ct.shape
    n = square.shape[0]
    span = v.shape[0]
    half = span // 2
    nh = n // 2
    row, col = lax.axis_index("row"), lax.axis_index("col")
    lo, core = row // 2, row % 2
    z = col * 2 + lo

    def place(dz, dc):
        zz, cc = (z + dz) % 4, (core + dc) % 2
        return (zz % 2) * 2 + cc, zz // 2

    def peer(dz, dc):
        r, c = place(dz, dc)
        return {"row": r, "col": c}

    def band(dz, dc):
        r, c = place(dz, dc)
        return rows_of((r * 2 + c) * width, width, 8)

    def remote(src, dst, send, recv, to):
        return pltpu.make_async_remote_copy(
            src_ref=src, dst_ref=dst, send_sem=send, recv_sem=recv, device_id=to, device_id_type=MESH
        )

    mine = band(0, 0)
    top_load = pltpu.make_async_copy(ct_hbm.at[:, pl.ds(0, n)], square.at[mine, :], load_sem.at[0])
    ct_load = pltpu.make_async_copy(ct_hbm, ct, load_sem.at[1])
    cr_load = pltpu.make_async_copy(
        ct_hbm.at[:, rows_of(row * span, span, 128)], cr.at[mine, :], load_sem.at[2]
    )
    v_load = pltpu.make_async_copy(v_hbm, v, load_sem.at[3])
    s_load = pltpu.make_async_copy(s_hbm, s, load_sem.at[4])
    for load in (top_load, ct_load, cr_load, v_load, s_load):
        load.start()

    barrier = pltpu.get_barrier_semaphore()
    for dz, dc in PEERS:
        pl.semaphore_signal(barrier, inc=1, device_id=peer(dz, dc), device_id_type=MESH)
    pl.semaphore_wait(barrier, len(PEERS))

    top_load.wait()
    def band_sizes(source_lo, step):
        for when, size in ((source_lo == 1, n), (source_lo * 2 + core == 0, B), (source_lo * 2 + core == 1, 2 * B)):
            @pl.when(when)
            def _():
                step(size)

    def top(i, size):
        block = square.at[mine, pl.ds(0, size)]
        return remote(block, block, top_s.at[i], top_r.at[i], peer(*FAR[i]))

    def top_in(i, size):
        block = square.at[band(-FAR[i][0], 0), pl.ds(0, size)]
        return remote(block, block, top_s.at[i], top_r.at[i], peer(*FAR[i]))

    def handed(i, size):
        block = square.at[band(-FAR[i][0] if i < 3 else 0, 0), pl.ds(0, size)]
        return remote(block, block, pass_s.at[i], pass_r.at[i], peer(0, 1))

    def got(i, size):
        block = square.at[band(-FAR[i][0] if i < 3 else 0, 1), pl.ds(0, size)]
        return remote(block, block, pass_s.at[i], pass_r.at[i], peer(0, 1))

    def source(i):
        return (lo + (FAR[i][0] if i < 3 else 0)) % 2

    def start_tops(size):
        for i in range(3):
            top(i, size).start()
        handed(3, size).start()

    band_sizes(lo, start_tops)

    ct_load.wait()
    quarter = half // 2
    cut = quarter + 2 * B
    cols = [[], [], []]
    for turn, size in enumerate((half, quarter, quarter)):
        for i, (dz, dc) in enumerate(PEERS):
            r, c = place(dz, dc)
            early = (r // 2) * c
            start = early * half if turn == 0 else (1 - early) * half + (turn - 1) * quarter
            cols[turn].append(remote(
                ct.at[:, rows_of(r * span + start, size, 128)], cr.at[mine, rows_of(start, size, 128)],
                col_s.at[turn, i], col_r.at[turn, i], peer(dz, dc),
            ))
    less = [
        remote(
            ct.at[:, pl.ds(n, half - n)], cr.at[mine, pl.ds(n, half - n)],
            col_s.at[0, i], col_r.at[0, i], peer(dz, dc),
        )
        for i, (dz, dc) in enumerate(PEERS)
    ]

    def first_turn(step, some=range(len(PEERS))):
        for i in some:
            r, _ = place(*PEERS[i])

            @pl.when(r == 0)
            def _():
                step(less[i])

            @pl.when(r != 0)
            def _():
                step(cols[0][i])


    v_load.wait()
    first, second = pl.ds(0, nh), pl.ds(nh, nh)
    to_core = remote(v.at[pl.ds(0, n), :], vt, vec_s.at[0], vec_r.at[0], {"row": 1, "col": col})
    to_first = remote(v.at[first, :], vt.at[first, :], vec_s.at[1], vec_r.at[1], {"row": 2, "col": col})
    to_second = remote(vt.at[second, :], vt.at[second, :], vec_s.at[1], vec_r.at[1], {"row": 3, "col": col})
    pass_first = remote(vt.at[first, :], vt.at[first, :], vec_s.at[0], vec_r.at[0], {"row": 3, "col": col})
    pass_second = remote(vt.at[second, :], vt.at[second, :], vec_s.at[0], vec_r.at[0], {"row": 2, "col": col})

    @pl.when(row == 0)
    def _():
        to_core.start()
        to_first.start()
        vt[...] = v[pl.ds(0, n), :]

    @pl.when(row == 1)
    def _():
        to_core.wait_recv()
        to_second.start()

    same = [i for i, (dz, _) in enumerate(PEERS) if dz % 2 == 0]
    apart = [i for i, (dz, _) in enumerate(PEERS) if dz % 2 == 1]
    for own_lo, order in ((0, (same, apart)), (1, (apart, same))):
        @pl.when(lo == own_lo)
        def _():
            for group in order:
                first_turn(lambda copy: copy.start(), group)
                for turn in (1, 2):
                    for i in group:
                        cols[turn][i].start()

    for i in range(3):
        def forward(size, i=i):
            top_in(i, size).wait_recv()
            handed(i, size).start()

        band_sizes(source(i), forward)

    for i in range(4):
        @pl.when(source(i) == 1)
        def _():
            got(i, n).wait_recv()

        @pl.when((source(i) == 0) & (core == 1))
        def _():
            got(i, B).wait_recv()

        @pl.when((source(i) == 0) & (core == 0))
        def _():
            got(i, 2 * B).wait_recv()

        band_sizes(source(i), lambda size, i=i: handed(i, size).wait_send())

    def end_tops(size):
        for i in range(3):
            top(i, size).wait_send()

    band_sizes(lo, end_tops)
    below = lax.broadcasted_iota(jnp.int32, (n, n), 0) >= lax.broadcasted_iota(jnp.int32, (n, n), 1)
    a[...] = jnp.where(below, square[...], square[...].T)

    cr_load.wait()

    @pl.when(row == 0)
    def _():
        cr[:, pl.ds(0, n)] = a[...]

    factor(a, e, d, f)

    @pl.when(row == 2)
    def _():
        to_first.wait_recv()
        pass_first.start()

    @pl.when(row == 3)
    def _():
        to_second.wait_recv()
        pass_second.start()

    s_load.wait()
    inverse = split(e[...])
    wh[...] = dot3(inverse, split(s[...]))

    @pl.when(row == 2)
    def _():
        pass_second.wait_recv()

    @pl.when(row == 3)
    def _():
        pass_first.wait_recv()

    y[...] = dot3(inverse, split(vt[...]))
    zv[...] = dot3(split(e[...].T), split(y[...]))

    left[pl.ds(0, nh), :] = e[rows_of((1 - lo) * nh, nh, 8), :]
    for j in range(2):
        left[pl.ds(nh + j * width, width), :] = e[band(0, j), :]

    @pl.when(row == 0)
    def _():
        for copy in less:
            copy.wait_recv()

    @pl.when(row != 0)
    def _():
        for copy in cols[0]:
            copy.wait_recv()

    early = lo * col
    base = row * span
    lefts = split(left[...])
    def back(dz, dc, kind, start, size):
        r, c = place(dz, dc)
        return remote(
            near.at[rows_of((r % 2) * 2 * width + c * width, width, 8), rows_of(start, size, 128)],
            ft.at[:, rows_of(base + start, size, 128)],
            back_s.at[kind, dc], back_r.at[kind, dc], peer(dz, dc),
        )

    short = [back(1, dc, 0, n, cut - n) for dc in range(2)]
    full = [back(1, dc, 0, 0, cut) for dc in range(2)]
    even = [back(3, dc, 1, cut, half - cut) for dc in range(2)]
    rest = [[back(3, dc, kind, kind * quarter, quarter) for dc in range(2)] for kind in (2, 3)]
    odd = [back(dz, dc, kind, col * half, half) for dc in range(2) for dz, kind in ((1, 0), (3, 1))]

    def on_kind(step):
        @pl.when(row == 0)
        def _():
            for copy in short + even:
                step(copy)

        @pl.when(row == 1)
        def _():
            for copy in full + even:
                step(copy)

        @pl.when(lo == 1)
        def _():
            for copy in odd:
                step(copy)

    def given(slot, start, size):
        out = ft.at[:, rows_of(base + start, size, 128)]
        return remote(own.at[:, rows_of(start, size, 128)], out, give_s.at[slot], give_r.at[slot], peer(0, 1))

    def factor_rows(slot, start, size):
        lanes, out = rows_of(start, size, 128), rows_of(base + start, size, 128)
        got = dot3(lefts, split(cr[:, lanes]))
        near[:, lanes] = got[:nh]
        ft[:, out] = got[nh:nh + width]
        own[:, lanes] = got[nh + width:]
        given(slot, start, size).start()

    factor_rows(0, early * half, half)
    on_kind(lambda copy: copy.start())

    step = 256

    zs = split(zv[...])

    def project(start, size):
        def one(i, _):
            part = rows_of(start + i * step, step, 128)
            pr[part, :] = v[part, :] - dot3(split(cr[:, part].T), zs)
            return 0

        lax.fori_loop(0, size // step, one, 0)

    def late(turn):
        return (1 - early) * half + (turn - 1) * quarter

    @pl.when(lo == 0)
    def _():
        for turn in (1, 2):
            for copy in cols[turn]:
                copy.wait_recv()
            factor_rows(turn, late(turn), quarter)
            for copy in rest[turn - 1]:
                copy.start()
        project(0, span)

    @pl.when(lo == 1)
    def _():
        project(early * half, half)
        for turn in (1, 2):
            for copy in cols[turn]:
                copy.wait_recv()
            factor_rows(turn, late(turn), quarter)
            project(late(turn), quarter)

    @pl.when(row == 0)
    def _():
        to_core.wait_send()
        to_first.wait_send()
        pr[pl.ds(0, n), :] = y[...]

    @pl.when(row == 1)
    def _():
        to_second.wait_send()

    @pl.when(row == 2)
    def _():
        pass_first.wait_send()

    @pl.when(row == 3)
    def _():
        pass_second.wait_send()

    first_turn(lambda copy: copy.wait_send())
    for copy in cols[1] + cols[2]:
        copy.wait_send()
    on_kind(lambda copy: copy.wait_send())

    @pl.when(lo == 0)
    def _():
        for copy in rest[0] + rest[1]:
            copy.wait_send()
        for copy in odd:
            copy.wait_recv()

    @pl.when(lo == 1)
    def _():
        @pl.when(core == 0)
        def _():
            short[0].wait_recv()
            full[1].wait_recv()

        @pl.when(core == 1)
        def _():
            full[0].wait_recv()
            short[1].wait_recv()

        for copy in even + rest[0] + rest[1]:
            copy.wait_recv()

    given(0, early * half, half).wait()
    for turn in (1, 2):
        given(turn, late(turn), quarter).wait()
    ft[:, pl.ds(0, n)] = a[mine, :]


def store(*refs):
    sems = refs[6]
    copies = [pltpu.make_async_copy(refs[i], refs[3 + i], sems.at[i]) for i in range(3)]
    for copy in copies:
        copy.start()
    for copy in copies:
        copy.wait()


def shards(foreground_cols, signal_rows, visibilities):
    length, width = foreground_cols.shape
    n = signal_rows.shape[0]
    span, vecs = visibilities.shape
    vmem = pl.BlockSpec(memory_space=pltpu.VMEM)
    hbm = pl.BlockSpec(memory_space=pl.ANY)
    dma = pltpu.SemaphoreType.DMA
    buffers = (
        (width, length), (n, span), signal_rows.shape, visibilities.shape, (n, vecs), (n, n), (n, n), (n, n),
        (B, B), (B, B), (n, vecs), (n, vecs), (n // 2 + 2 * width, n), (n // 2, span), (width, span),
    )
    ft, whitened, projected = pl.pallas_call(
        kernel,
        name="whiten",
        out_shape=[
            pltpu.VMEM((width, length), F32),
            pltpu.VMEM(signal_rows.shape, F32),
            pltpu.VMEM(visibilities.shape, F32),
        ],
        in_specs=[hbm] * 3,
        out_specs=[vmem] * 3,
        scratch_shapes=[pltpu.VMEM(shape, F32) for shape in buffers]
        + [dma(k) for k in ((5,), (3,), (3,), (4,), (4,), (3, 7), (3, 7), (3,), (2,), (4, 2), (4, 2), (3,), (3,))],
        compiler_params=pltpu.CompilerParams(
            collective_id=0, has_side_effects=True, vmem_limit_bytes=56 * 1024 * 1024
        ),
    )(foreground_cols.T, signal_rows, visibilities)
    ft, whitened, projected = pl.pallas_call(
        store,
        name="store",
        out_shape=[jax.ShapeDtypeStruct(x.shape, F32) for x in (ft, whitened, projected)],
        in_specs=[vmem] * 3,
        out_specs=[hbm] * 3,
        scratch_shapes=[dma((3,))],
        compiler_params=pltpu.CompilerParams(vmem_limit_bytes=1024 * 1024),
    )(ft, whitened, projected)
    return ft.T, whitened, projected


def solution(mesh):
    return jax.shard_map(
        shards,
        mesh=mesh,
        in_specs=(P("ma", ("row", "col")), P("ma", ("row", "col")), P(("ma", "row"), "col")),
        out_specs=(P("ma", ("row", "col")), P("ma", ("row", "col")), P(("ma", "row"), "col")),
        check_vma=False,
    )
```
